32 devices in a mesh: rows: 8 (over z, y), model: 4 (over x, core).
Axes of the slice: x: 2, y: 2, z: 4, core: 2. Of those that a mesh axis runs over, the one named last changes fastest.
Arguments:
- w_query: float32 [4096, 4096], P('rows', 'model'), may hold values from -0.125 to 0.125
- first_query: float32 [4096, 4096], P('rows', 'model'), may hold values from -6 to 6
- second_query: float32 [4096, 4096], P('rows', 'model'), may hold values from 0.1 to 10
- w_key: float32 [4096, 1024], P('rows', 'model'), may hold values from -0.125 to 0.125
- first_key: float32 [4096, 1024], P('rows', 'model'), may hold values from -6 to 6
- second_key: float32 [4096, 1024], P('rows', 'model'), may hold values from 0.1 to 10
- w_value: float32 [4096, 1024], P('rows', 'model'), may hold values from -0.125 to 0.125
- first_value: float32 [4096, 1024], P('rows', 'model'), may hold values from -6 to 6
- second_value: float32 [4096, 1024], P('rows', 'model'), may hold values from 0.1 to 10
- norm_train: float32 [4096], P(('rows', 'model')), may hold values from 0.25 to 1.75
- norm_step: float32 [4096], P(('rows', 'model')), may hold values from -0.3 to 0.3
Outputs:
- final_query: bfloat16 [4096, 4096], P(None, 'model')
- final_key: bfloat16 [4096, 1024], P(None, 'model')
- final_value: bfloat16 [4096, 1024], P(None, 'model')
- column_query: float32 [4096], P('model')
- column_key: float32 [1024], P('model')
- column_value: float32 [1024], P('model')
- serve_norm: bfloat16 [4096], replicated
- result_query: float32 [4096, 4096], P('rows', 'model')
- result_key: float32 [4096, 1024], P('rows', 'model')
- result_value: float32 [4096, 1024], P('rows', 'model')
The draws below stay inside these ranges and needn't reach their ends.
All inputs are finite; a program needn't handle non-finite values. Where the reference program divides by a largest or mean magnitude, that divisor is 1e-20 or more.
Results may differ from the reference program's by a relative error of at most 0.0004.
Values may be sent and summed in bfloat16 or wider, within the bound.
A program may use at most 64 MiB of HBM per device.

```python
import math
import jax
import jax.numpy as jnp
from jax import lax

D_MODEL = 4096
Q_DIM = 4096
KV_DIM = 1024


def strengthened(values, key, source, target, shards_of, factor):
    def block_of(dim):
        return (jnp.arange(values.shape[dim]) // (values.shape[dim] // shards_of)).reshape((-1,) + (1,) * (values.ndim - 1 - dim))

    first = jax.random.permutation(key, shards_of)[block_of(target)]
    second = (block_of(target) + shards_of // 2) % shards_of
    return jnp.where((block_of(source) == first) | (block_of(source) == second), factor * values, values)


def steps_of(rng, shape, split, low, largest):
    loudness = 1.0
    for position, parts in split:
        draws = jax.random.uniform(jax.random.fold_in(jax.random.fold_in(rng, 6), position), (parts,), jnp.float32, low / len(split), largest / len(split))
        loudness = loudness * jnp.repeat(jnp.exp(draws), shape[position] // parts).reshape((-1,) + (1,) * (len(shape) - 1 - position))
    return loudness


def gaussian(key, shape, spread, bound, cuts=(), held_as=jnp.bfloat16):
    array = jax.random.normal(key, shape, jnp.float32) * spread
    if len(cuts) > 0:
        array = steps_of(key, shape, cuts, -0.22, 0.18) * array
    return jnp.clip(array, min=-bound, max=bound).astype(held_as)


def noise_with(rng, dims, width, most, cuts, heavy, held_as=jnp.bfloat16):
    array = width * jax.random.normal(rng, dims, jnp.float32)
    if cuts:
        array = array * steps_of(rng, dims, cuts, -0.22, 0.18)
    return jnp.clip(strengthened(array, jax.random.fold_in(rng, 3), *heavy), -most, most).astype(held_as)


def setup_inputs(seed: int = 0) -> dict:
    seeds = jax.random.split(jax.random.key(seed), 12)
    w_query = noise_with(seeds[0], (D_MODEL, Q_DIM), D_MODEL ** -0.5, 0.125, ((0, 8), (1, 4)), (0, 1, 8, 2.0), jnp.float32)
    first_query = gaussian(seeds[1], (D_MODEL, Q_DIM), 1.0, 6.0, ((0, 8), (1, 4)), jnp.float32)
    second_query = jnp.clip(jnp.exp(math.log(10.0) - 4.6051702 * jax.random.uniform(seeds[2], (D_MODEL, Q_DIM), jnp.float32) ** steps_of(seeds[2], (D_MODEL, Q_DIM), ((0, 8), (1, 4)), -0.2, 0.2)), 0.1, 10.0)
    w_key = noise_with(seeds[3], (D_MODEL, KV_DIM), D_MODEL ** -0.5, 0.125, ((0, 8), (1, 4)), (0, 1, 8, 2.0), jnp.float32)
    first_key = gaussian(seeds[4], (D_MODEL, KV_DIM), 1.0, 6.0, ((0, 8), (1, 4)), jnp.float32)
    second_key = jnp.clip(jnp.exp(math.log(10.0) - 4.6051702 * jax.random.uniform(seeds[5], (D_MODEL, KV_DIM), jnp.float32) ** steps_of(seeds[5], (D_MODEL, KV_DIM), ((0, 8), (1, 4)), -0.2, 0.2)), 0.1, 10.0)
    w_value = noise_with(seeds[6], (D_MODEL, KV_DIM), D_MODEL ** -0.5, 0.125, ((0, 8), (1, 4)), (0, 1, 8, 2.0), jnp.float32)
    first_value = gaussian(seeds[7], (D_MODEL, KV_DIM), 1.0, 6.0, ((0, 8), (1, 4)), jnp.float32)
    second_value = jnp.clip(jnp.exp(math.log(10.0) - 4.6051702 * jax.random.uniform(seeds[8], (D_MODEL, KV_DIM), jnp.float32) ** steps_of(seeds[8], (D_MODEL, KV_DIM), ((0, 8), (1, 4)), -0.2, 0.2)), 0.1, 10.0)
    norm_train = jnp.clip(1.0 + 0.15 * jax.random.normal(seeds[9], (D_MODEL,), jnp.float32), 0.25, 1.75)
    norm_step = jnp.clip(jax.random.uniform(seeds[10], (D_MODEL,), jnp.float32, -0.3, 0.3) * steps_of(seeds[10], (D_MODEL,), ((0, 32),), -0.4, 0.0), -0.3, 0.3)
    return dict(w_query=w_query, first_query=first_query, second_query=second_query, w_key=w_key, first_key=first_key, second_key=second_key, w_value=w_value, first_value=first_value, second_value=second_value, norm_train=norm_train, norm_step=norm_step)


learn_rate = 0.01
decay_rate = 0.05
tiny_value = 1e-08

def reference(w_query, first_query, second_query, w_key, first_key, second_key, w_value, first_value, second_value, norm_train, norm_step):
    result_query = w_query - learn_rate * (first_query / (jnp.sqrt(second_query) + tiny_value) + decay_rate * w_query)
    result_key = w_key - learn_rate * (first_key / (jnp.sqrt(second_key) + tiny_value) + decay_rate * w_key)
    result_value = w_value - learn_rate * (first_value / (jnp.sqrt(second_value) + tiny_value) + decay_rate * w_value)
    column_query = lax.optimization_barrier(jnp.sum(jnp.abs(result_query), axis=0)) / D_MODEL
    final_query = (result_query / column_query).astype(jnp.bfloat16)
    column_key = lax.optimization_barrier(jnp.sum(jnp.abs(result_key), axis=0)) / D_MODEL
    final_key = (result_key / column_key).astype(jnp.bfloat16)
    column_value = lax.optimization_barrier(jnp.sum(jnp.abs(result_value), axis=0)) / D_MODEL
    final_value = (result_value / column_value).astype(jnp.bfloat16)
    serve_norm = (norm_train + norm_step).astype(jnp.bfloat16)
    return (final_query, final_key, final_value, column_query, column_key, column_value, serve_norm, result_query, result_key, result_value)
```

```python
import functools

import jax
import jax.numpy as jnp
from jax import lax
from jax.experimental import pallas as pl
from jax.experimental.pallas import tpu as pltpu
from jax.sharding import PartitionSpec as P

learn_rate = 0.01
decay_rate = 0.05
tiny_value = 1e-08

MESH = pl.DeviceIdType.MESH
SIDE = 2
TILE = 32
PIECES = 4


def adam(w, first, second):
    return w - learn_rate * (first / (jnp.sqrt(second) + tiny_value) + decay_rate * w)


def plain(d_model, arrays):
    *weights, norm_train, norm_step = arrays
    results = [adam(*weights[3 * i : 3 * i + 3]) for i in range(3)]
    totals = lax.psum(tuple(jnp.sum(jnp.abs(r), axis=0) for r in results), "rows")
    columns = [t / d_model for t in totals]
    finals = [
        lax.all_gather((r / c).astype(jnp.bfloat16), "rows", axis=0, tiled=True)
        for r, c in zip(results, columns)
    ]
    serve = lax.all_gather(
        (norm_train + norm_step).astype(jnp.bfloat16), ("rows", "model"), axis=0, tiled=True
    )
    return (*finals, *columns, serve, *results)


def kernel(
    n_rows, n_model, blocks, d_model,
    *refs,
):
    ins, refs = refs[:9], refs[9:]
    nt_ref, ns_ref = refs[:2]
    finals, cols, norm_out, results = refs[2:5], refs[5:8], refs[8], refs[9:12]
    bufs = refs[12:15]
    (norms, sums, gains, in_sem, norm_sem, sum_send, sum_recv, gain_send, gain_recv,
     up_send, down_send, side_send, line_recv, side_recv) = refs[15:]

    line = n_rows // SIDE
    me = lax.axis_index("rows")
    col = lax.axis_index("model")
    z, y = me // SIDE, me % SIDE
    other = 1 - y
    share = bufs[0].shape[1]
    nb = len(blocks)
    lead = nb - 1

    barrier = pltpu.get_barrier_semaphore()
    for k in range(1, n_rows):
        pl.semaphore_signal(
            barrier, inc=1, device_id={"rows": lax.rem(me + k, n_rows)}, device_id_type=MESH
        )
    for k in range(1, n_model):
        pl.semaphore_signal(
            barrier, inc=1, device_id={"model": lax.rem(col + k, n_model)}, device_id_type=MESH
        )

    def load(b):
        a, start, width = blocks[b]
        where = (slice(None), pl.ds(start, width))
        for k in range(3):
            pltpu.make_async_copy(
                ins[3 * a + k].at[where], bufs[a].at[(k, *where)], in_sem.at[b]
            ).start()

    def wait_bytes(ref, sem):
        pltpu.make_async_copy(ref, ref, sem).wait()

    def step(b):
        a, start, width = blocks[b]
        wait_bytes(bufs[a].at[:, :, pl.ds(start, width)], in_sem.at[b])
        if b == 0:
            for other_b in order[1:]:
                load(other_b)
            for n, ref in enumerate((nt_ref, ns_ref)):
                pltpu.make_async_copy(ref, norms.at[n], norm_sem.at[0]).start()

        def one(i, acc):
            rows = pl.ds(pl.multiple_of(i * TILE, TILE), TILE)
            where = (rows, pl.ds(start, width))
            r = adam(*(bufs[a][(k, *where)] for k in range(3)))
            results[a][where] = r
            m = jnp.abs(r).reshape(TILE // 8, 8, width)
            return acc + jnp.sum(m, axis=0)

        acc = lax.fori_loop(0, share // TILE, one, jnp.zeros((8, width), jnp.float32))
        sums[b, me] = jnp.sum(acc, axis=0, keepdims=True)

    def sum_copy(b, k):
        return pltpu.make_async_remote_copy(
            src_ref=sums.at[b, me],
            dst_ref=sums.at[b, me],
            send_sem=sum_send.at[0],
            recv_sem=sum_recv.at[b],
            device_id={"rows": lax.rem(me + k, n_rows)},
            device_id_type=MESH,
        )

    def place(j, owner):
        a, start, width = blocks[j]
        rows = pl.ds(pl.multiple_of(owner * share, share), share)
        return finals[a].at[rows, pl.ds(start, width)]

    def some(n):
        w = finals[0].shape[1]
        return finals[0].at[pl.ds(0, n * share * blocks[0][2] // w)]

    def to_line(zs, j, up, to):
        owner = zs * SIDE + (other if j == nb else y)
        part = place(min(j, lead), owner)
        slot = jnp.where(zs < to, zs, zs - 1)
        return pltpu.make_async_remote_copy(
            src_ref=part,
            dst_ref=part,
            send_sem=(up_send if up else down_send).at[zs],
            recv_sem=line_recv.at[slot, j],
            device_id={"rows": me + (SIDE if up else -SIDE)},
            device_id_type=MESH,
        )

    def to_side(zs, j, mine=True):
        part = place(j, zs * SIDE + (y if mine else other))
        return pltpu.make_async_remote_copy(
            src_ref=part,
            dst_ref=part,
            send_sem=side_send.at[0],
            recv_sem=side_recv.at[1 if j == lead else 0],
            device_id={"rows": z * SIDE + other},
            device_id_type=MESH,
        )

    def both_ways(zs, j):
        @pl.when(z > 0)
        def _():
            to_line(zs, j, False, z - 1).start()

        @pl.when(z < line - 1)
        def _():
            to_line(zs, j, True, z + 1).start()

    def gain_model(k):
        return pltpu.make_async_remote_copy(
            src_ref=gains.at[me, col],
            dst_ref=gains.at[me, col],
            send_sem=gain_send.at[0],
            recv_sem=gain_recv.at[0],
            device_id={"model": lax.rem(col + k, n_model)},
            device_id_type=MESH,
        )

    def gain_rows(k):
        return pltpu.make_async_remote_copy(
            src_ref=gains.at[me],
            dst_ref=gains.at[me],
            send_sem=gain_send.at[1],
            recv_sem=gain_recv.at[1],
            device_id={"rows": lax.rem(me + k, n_rows)},
            device_id_type=MESH,
        )

    order = [0, lead] + list(range(1, lead))
    load(0)
    for i, b in enumerate(order):
        step(b)
        if i == 0:
            pl.semaphore_wait(barrier, n_rows + n_model - 2)
        for k in range(1, n_rows):
            sum_copy(b, k).start()
    wait_bytes(norms, norm_sem.at[0])
    gains[me, col] = norms[0] + norms[1]
    for k in range(1, n_model):
        gain_model(k).start()

    for b in order:
        a, start, width = blocks[b]
        wait_bytes(sums.at[b, pl.ds(0, n_rows - 1)], sum_recv.at[b])
        total = sums[b, 0]
        for k in range(1, n_rows):
            total = total + sums[b, k]
        column = total / d_model
        cols[a][:, pl.ds(start, width)] = column
        scale = jnp.broadcast_to(1.0 / column, (TILE, width))

        def one(i, carry):
            rows = pl.ds(pl.multiple_of(i * TILE, TILE), TILE)
            there = pl.ds(pl.multiple_of(me * share + i * TILE, TILE), TILE)
            where = pl.ds(start, width)
            finals[a][there, where] = (results[a][rows, where] * scale).astype(jnp.bfloat16)
            return carry

        lax.fori_loop(0, share // TILE, one, 0)
        if b != lead:
            both_ways(z, b)
        to_side(z, b).start()
    both_ways(z, lead)

    wait_bytes(gains.at[0, pl.ds(0, n_model - 1)], gain_recv.at[0])
    for k in range(1, n_rows):
        gain_rows(k).start()

    to_side(z, lead, False).wait_recv()
    both_ways(z, nb)

    wait_bytes(gains.at[pl.ds(0, n_rows - 1)], gain_recv.at[1])
    for r in range(n_rows):
        for m in range(n_model):
            norm_out[pl.ds(r * n_model + m, 1), :] = gains[r, m]

    for d in range(1, line):
        for j in range(nb + 1):

            @pl.when(z - d >= 0)
            def _():
                to_line(z - d, j, True, z).wait_recv()

                @pl.when(z < line - 1)
                def _():
                    to_line(z - d, j, True, z + 1).start()

                if j < lead:
                    to_side(z - d, j).start()

            @pl.when(z + d < line)
            def _():
                to_line(z + d, j, False, z).wait_recv()

                @pl.when(z > 0)
                def _():
                    to_line(z + d, j, False, z - 1).start()

                if j < lead:
                    to_side(z + d, j).start()

    wait_bytes(gains.at[0, pl.ds(0, n_model - 1)], gain_send.at[0])
    wait_bytes(gains.at[pl.ds(0, n_rows - 1)], gain_send.at[1])
    wait_bytes(sums.at[:, pl.ds(0, n_rows - 1)], sum_send.at[0])
    for zs in range(line):

        @pl.when((z > 0) & (z <= zs))
        def _():
            wait_bytes(some(nb + 1), down_send.at[zs])

        @pl.when((z < line - 1) & (z >= zs))
        def _():
            wait_bytes(some(nb + 1), up_send.at[zs])

    wait_bytes(some(line * lead), side_recv.at[0])
    wait_bytes(some(line * lead + 1), side_send.at[0])


def write(pieces, *refs):
    ins, outs, sem = refs[:10], refs[10:20], refs[20]
    copies = []
    for n, (i, start, rows) in enumerate(pieces):
        where = pl.ds(start, rows)
        c = pltpu.make_async_copy(ins[i].at[where], outs[i].at[where], sem.at[n])
        c.start()
        copies.append(c)
    outs[6][...] = ins[6][...].astype(jnp.bfloat16)
    for c in copies:
        c.wait()


def fused(n_rows, n_model, d_model, blocks, arrays):
    *weights, norm_train, norm_step = arrays
    share = weights[0].shape[0]
    widths = [weights[3 * a].shape[1] for a in range(3)]
    line, nb = n_rows // SIDE, len(blocks)
    unit = norm_train.shape[0]
    anywhere = pl.BlockSpec(memory_space=pl.ANY)
    vmem = pl.BlockSpec(memory_space=pltpu.VMEM)
    f32, dma = jnp.float32, pltpu.SemaphoreType.DMA
    out = pl.pallas_call(
        functools.partial(kernel, n_rows, n_model, blocks, d_model),
        out_shape=[
            *(pltpu.VMEM((d_model, w), jnp.bfloat16) for w in widths),
            *(pltpu.VMEM((1, w), f32) for w in widths),
            pltpu.VMEM((n_rows * n_model, unit), f32),
            *(pltpu.VMEM((share, w), f32) for w in widths),
        ],
        in_specs=[anywhere] * 11,
        out_specs=[vmem] * 10,
        scratch_shapes=[
            *(pltpu.VMEM((3, share, w), f32) for w in widths),
            pltpu.VMEM((2, 1, unit), f32),
            pltpu.VMEM((nb, n_rows, 1, blocks[0][2]), f32),
            pltpu.VMEM((n_rows, n_model, 1, unit), f32),
            dma((nb,)),
            dma((1,)),
            dma((1,)),
            dma((nb,)),
            dma((2,)),
            dma((2,)),
            dma((line,)),
            dma((line,)),
            dma((1,)),
            dma((line - 1, nb + 1)),
            dma((2,)),
        ],
        compiler_params=pltpu.CompilerParams(
            collective_id=0, has_side_effects=True, vmem_limit_bytes=48 * 2**20
        ),
    )(*weights, norm_train.reshape(1, -1), norm_step.reshape(1, -1))
    pieces = []
    for i in [0, 7, 1, 2, 8, 9, 3, 4, 5]:
        rows = out[i].shape[0]
        cut = rows // PIECES if i == 0 else rows
        pieces += [(i, r, cut) for r in range(0, rows, cut)]
    done = pl.pallas_call(
        functools.partial(write, pieces),
        out_shape=[
            jax.ShapeDtypeStruct(o.shape, jnp.bfloat16 if i == 6 else o.dtype)
            for i, o in enumerate(out)
        ],
        in_specs=[vmem if i == 6 else anywhere for i in range(10)],
        out_specs=[vmem if i == 6 else anywhere for i in range(10)],
        scratch_shapes=[dma((len(pieces),))],
        compiler_params=pltpu.CompilerParams(vmem_limit_bytes=2**20),
    )(*out)
    return tuple(d.reshape(-1) if 3 <= i <= 6 else d for i, d in enumerate(done))


def solution(mesh):
    n_rows, n_model = mesh.shape["rows"], mesh.shape["model"]

    def body(*arrays):
        share = arrays[0].shape[0]
        widths = [arrays[3 * a].shape[1] for a in range(3)]
        width = min(widths)
        d_model = share * n_rows
        fits = (
            n_rows % SIDE == 0
            and 2 <= n_rows // SIDE <= 4
            and share % TILE == 0
            and width % 128 == 0
            and all(w % width == 0 for w in widths)
            and sum(widths) + width <= 2 * widths[0]
        )
        if not fits:
            return plain(d_model, arrays)
        blocks = tuple(
            (a, s, width) for a, w in enumerate(widths) for s in range(0, w, width)
        )
        return fused(n_rows, n_model, d_model, blocks, arrays)

    return jax.shard_map(
        body,
        mesh=mesh,
        in_specs=(P("rows", "model"),) * 9 + (P(("rows", "model")),) * 2,
        out_specs=(
            *(P(None, "model"),) * 3,
            *(P("model"),) * 3,
            P(),
            *(P("rows", "model"),) * 3,
        ),
        check_vma=False,
    )
```

```python
import functools

import jax
import jax.numpy as jnp
from jax import lax
from jax.experimental import pallas as pl
from jax.experimental.pallas import tpu as pltpu
from jax.sharding import PartitionSpec as P

learn_rate = 0.01
decay_rate = 0.05
tiny_value = 1e-08

MESH = pl.DeviceIdType.MESH
SIDE = 2
TILE = 32
PIECES = 4
EARLY = 128


def adam(w, first, second):
    return w - learn_rate * (first / (jnp.sqrt(second) + tiny_value) + decay_rate * w)


def plain(d_model, arrays):
    *weights, norm_train, norm_step = arrays
    results = [adam(*weights[3 * i : 3 * i + 3]) for i in range(3)]
    totals = lax.psum(tuple(jnp.sum(jnp.abs(r), axis=0) for r in results), "rows")
    columns = [t / d_model for t in totals]
    finals = [
        lax.all_gather((r / c).astype(jnp.bfloat16), "rows", axis=0, tiled=True)
        for r, c in zip(results, columns)
    ]
    serve = lax.all_gather(
        (norm_train + norm_step).astype(jnp.bfloat16), ("rows", "model"), axis=0, tiled=True
    )
    return (*finals, *columns, serve, *results)


def kernel(
    n_rows, n_model, blocks, d_model,
    *refs,
):
    ins, refs = refs[:9], refs[9:]
    nt_ref, ns_ref = refs[:2]
    finals, cols, norm_out, results = refs[2:5], refs[5:8], refs[8], refs[9:12]
    bufs = refs[12:15]
    (norms, lines, sums, gains, in_sem, norm_sem, sum_send, sum_recv, gain_send, gain_recv,
     up_send, down_send, side_send, line_recv, side_recv, own_send, early, early_send, early_recv) = refs[15:]

    line = n_rows // SIDE
    me = lax.axis_index("rows")
    col = lax.axis_index("model")
    z, y = me // SIDE, me % SIDE
    other = 1 - y
    share = bufs[0].shape[1]
    nb = len(blocks)
    lead = nb - 1

    barrier = pltpu.get_barrier_semaphore()
    for k in range(1, n_rows):
        pl.semaphore_signal(
            barrier, inc=1, device_id={"rows": lax.rem(me + k, n_rows)}, device_id_type=MESH
        )
    for k in range(1, n_model):
        pl.semaphore_signal(
            barrier, inc=1, device_id={"model": lax.rem(col + k, n_model)}, device_id_type=MESH
        )

    def load(b):
        a, start, width = blocks[b]
        where = (slice(None), pl.ds(start, width))
        for k in range(3):
            pltpu.make_async_copy(
                ins[3 * a + k].at[where], bufs[a].at[(k, *where)], in_sem.at[b]
            ).start()

    def wait_bytes(ref, sem):
        pltpu.make_async_copy(ref, ref, sem).wait()

    def step(b):
        a, start, width = blocks[b]
        wait_bytes(bufs[a].at[:, :, pl.ds(start, width)], in_sem.at[b])
        if b == 0:
            for other_b in order[1:]:
                load(other_b)
            for n, ref in enumerate((nt_ref, ns_ref)):
                pltpu.make_async_copy(ref, norms.at[n], norm_sem.at[0]).start()

        def one(i, acc):
            rows = pl.ds(pl.multiple_of(i * TILE, TILE), TILE)
            where = (rows, pl.ds(start, width))
            r = adam(*(bufs[a][(k, *where)] for k in range(3)))
            results[a][where] = r
            m = jnp.abs(r).reshape(TILE // 8, 8, width)
            return acc + jnp.sum(m, axis=0)

        acc = lax.fori_loop(0, share // TILE, one, jnp.zeros((8, width), jnp.float32))
        sums[b, me] = jnp.sum(acc, axis=0, keepdims=True)

    def sum_copy(b, k):
        return pltpu.make_async_remote_copy(
            src_ref=sums.at[b, me],
            dst_ref=sums.at[b, me],
            send_sem=sum_send.at[0],
            recv_sem=sum_recv.at[b],
            device_id={"rows": lax.rem(me + k, n_rows)},
            device_id_type=MESH,
        )

    def place(j, owner, late=False):
        a, start, width = blocks[j]
        skip = EARLY if late and j == 0 else 0
        rows = pl.ds(pl.multiple_of(owner * share + skip, 16), share - skip)
        return finals[a].at[rows, pl.ds(start, width)]

    def some(n, late=False):
        rows = n * share - (EARLY if late else 0)
        return finals[0].at[pl.ds(0, rows * blocks[0][2] // finals[0].shape[1])]

    def early_copy(n, to):
        return pltpu.make_async_remote_copy(
            src_ref=results[0].at[pl.ds(0, EARLY), pl.ds(0, blocks[0][2])],
            dst_ref=early.at[n],
            send_sem=early_send.at[n],
            recv_sem=early_recv.at[n],
            device_id={"rows": to},
            device_id_type=MESH,
        )

    def to_line(zs, j, up, to, late=False, own=False):
        owner = zs * SIDE + (other if j == nb else y)
        part = place(min(j, lead), owner, late)
        slot = jnp.where(zs < to, zs, zs - 1)
        return pltpu.make_async_remote_copy(
            src_ref=part,
            dst_ref=part,
            send_sem=own_send.at[int(up)] if own else (up_send if up else down_send).at[zs],
            recv_sem=line_recv.at[slot, j],
            device_id={"rows": me + (SIDE if up else -SIDE)},
            device_id_type=MESH,
        )

    def to_side(zs, j, mine=True, late=False):
        part = place(j, zs * SIDE + (y if mine else other), late)
        return pltpu.make_async_remote_copy(
            src_ref=part,
            dst_ref=part,
            send_sem=side_send.at[0],
            recv_sem=side_recv.at[1 if j == lead else 0],
            device_id={"rows": z * SIDE + other},
            device_id_type=MESH,
        )

    def both_ways(j):
        @pl.when(z > 0)
        def _():
            to_line(z, j, False, z - 1, True, True).start()

        @pl.when(z < line - 1)
        def _():
            to_line(z, j, True, z + 1, True, True).start()

    def gain_model(k):
        return pltpu.make_async_remote_copy(
            src_ref=gains.at[me, col],
            dst_ref=gains.at[me, col],
            send_sem=gain_send.at[0],
            recv_sem=gain_recv.at[0],
            device_id={"model": lax.rem(col + k, n_model)},
            device_id_type=MESH,
        )

    def gain_rows(k):
        return pltpu.make_async_remote_copy(
            src_ref=gains.at[me],
            dst_ref=gains.at[me],
            send_sem=gain_send.at[1],
            recv_sem=gain_recv.at[1],
            device_id={"rows": lax.rem(me + k, n_rows)},
            device_id_type=MESH,
        )

    order = [0, lead] + list(range(1, lead))
    load(0)
    for i, b in enumerate(order):
        step(b)
        if i == 0:
            pl.semaphore_wait(barrier, n_rows + n_model - 2)
        for k in range(1, n_rows):
            sum_copy(b, k).start()
        if i == 0:
            early_copy(0, z * SIDE + other).start()

            @pl.when(z < line - 1)
            def _():
                early_copy(1, me + SIDE).start()

            @pl.when(z > 0)
            def _():
                early_copy(2, me - SIDE).start()
    wait_bytes(norms, norm_sem.at[0])
    gains[me, col] = norms[0] + norms[1]
    for k in range(1, n_model):
        gain_model(k).start()

    for b in order:
        a, start, width = blocks[b]
        wait_bytes(sums.at[b, pl.ds(0, n_rows - 1)], sum_recv.at[b])
        total = sums[b, 0]
        for k in range(1, n_rows):
            total = total + sums[b, k]
        column = total / d_model
        cols[a][:, pl.ds(start, width)] = column
        scale = jnp.broadcast_to(1.0 / column, (TILE, width))

        def one(i, carry):
            rows = pl.ds(pl.multiple_of(i * TILE, TILE), TILE)
            there = pl.ds(pl.multiple_of(me * share + i * TILE, TILE), TILE)
            where = pl.ds(start, width)
            finals[a][there, where] = (results[a][rows, where] * scale).astype(jnp.bfloat16)
            return carry

        lax.fori_loop(0, share // TILE, one, 0)
        if b != lead:
            both_ways(b)
        to_side(z, b, late=True).start()
    both_ways(lead)

    width = blocks[0][2]
    scale = jnp.broadcast_to(1.0 / cols[0][:, pl.ds(0, width)], (TILE, width))

    def finish(n, owner):
        early_copy(n, owner).wait_recv()

        def one(i, carry):
            rows = pl.ds(pl.multiple_of(i * TILE, TILE), TILE)
            there = pl.ds(pl.multiple_of(owner * share + i * TILE, TILE), TILE)
            finals[0][there, pl.ds(0, width)] = (early[n, rows] * scale).astype(jnp.bfloat16)
            return carry

        lax.fori_loop(0, EARLY // TILE, one, 0)

    @pl.when(z > 0)
    def _():
        finish(1, me - SIDE)

    @pl.when(z < line - 1)
    def _():
        finish(2, me + SIDE)

    finish(0, z * SIDE + other)

    wait_bytes(gains.at[0, pl.ds(0, n_model - 1)], gain_recv.at[0])
    for k in range(1, n_rows):
        gain_rows(k).start()

    to_side(z, lead, False).wait_recv()
    both_ways(nb)

    wait_bytes(gains.at[pl.ds(0, n_rows - 1)], gain_recv.at[1])
    for r in range(n_rows):
        for m in range(n_model):
            lines[pl.ds(r * n_model + m, 1), :] = gains[r, m]
    norm_out[...] = lines[...].astype(jnp.bfloat16)

    for d in range(1, line):
        for j in range(nb + 1):

            @pl.when(z - d >= 0)
            def _():
                to_line(z - d, j, True, z, d == 1).wait_recv()

                @pl.when(z < line - 1)
                def _():
                    to_line(z - d, j, True, z + 1).start()

                if j < lead:
                    to_side(z - d, j).start()

            @pl.when(z + d < line)
            def _():
                to_line(z + d, j, False, z, d == 1).wait_recv()

                @pl.when(z > 0)
                def _():
                    to_line(z + d, j, False, z - 1).start()

                if j < lead:
                    to_side(z + d, j).start()

    wait_bytes(gains.at[0, pl.ds(0, n_model - 1)], gain_send.at[0])
    wait_bytes(gains.at[pl.ds(0, n_rows - 1)], gain_send.at[1])
    wait_bytes(sums.at[:, pl.ds(0, n_rows - 1)], sum_send.at[0])
    early_copy(0, me).wait_send()

    @pl.when(z < line - 1)
    def _():
        early_copy(1, me).wait_send()
        wait_bytes(some(nb + 1, True), own_send.at[1])

    @pl.when(z > 0)
    def _():
        early_copy(2, me).wait_send()
        wait_bytes(some(nb + 1, True), own_send.at[0])

    for zs in range(line):

        @pl.when((z > 0) & (z < zs))
        def _():
            wait_bytes(some(nb + 1), down_send.at[zs])

        @pl.when((z < line - 1) & (z > zs))
        def _():
            wait_bytes(some(nb + 1), up_send.at[zs])

    wait_bytes(some(line * lead, True), side_recv.at[0])
    wait_bytes(some(line * lead + 1, True), side_send.at[0])


def write(pieces, *refs):
    ins, outs, sem = refs[:10], refs[10:20], refs[20]
    copies = []
    for n, (i, start, rows) in enumerate(pieces):
        where = pl.ds(start, rows)
        c = pltpu.make_async_copy(ins[i].at[where], outs[i].at[where], sem.at[n])
        c.start()
        copies.append(c)
    for c in copies:
        c.wait()


def fused(n_rows, n_model, d_model, blocks, arrays):
    *weights, norm_train, norm_step = arrays
    share = weights[0].shape[0]
    widths = [weights[3 * a].shape[1] for a in range(3)]
    line, nb = n_rows // SIDE, len(blocks)
    unit = norm_train.shape[0]
    anywhere = pl.BlockSpec(memory_space=pl.ANY)
    vmem = pl.BlockSpec(memory_space=pltpu.VMEM)
    f32, dma = jnp.float32, pltpu.SemaphoreType.DMA
    out = pl.pallas_call(
        functools.partial(kernel, n_rows, n_model, blocks, d_model),
        out_shape=[
            *(pltpu.VMEM((d_model, w), jnp.bfloat16) for w in widths),
            *(pltpu.VMEM((1, w), f32) for w in widths),
            pltpu.VMEM((n_rows * n_model, unit), jnp.bfloat16),
            *(pltpu.VMEM((share, w), f32) for w in widths),
        ],
        in_specs=[anywhere] * 11,
        out_specs=[vmem] * 10,
        scratch_shapes=[
            *(pltpu.VMEM((3, share, w), f32) for w in widths),
            pltpu.VMEM((2, 1, unit), f32),
            pltpu.VMEM((n_rows * n_model, unit), f32),
            pltpu.VMEM((nb, n_rows, 1, blocks[0][2]), f32),
            pltpu.VMEM((n_rows, n_model, 1, unit), f32),
            dma((nb,)),
            dma((1,)),
            dma((1,)),
            dma((nb,)),
            dma((2,)),
            dma((2,)),
            dma((line,)),
            dma((line,)),
            dma((1,)),
            dma((line - 1, nb + 1)),
            dma((2,)),
            dma((2,)),
            pltpu.VMEM((3, EARLY, blocks[0][2]), f32),
            dma((3,)),
            dma((3,)),
        ],
        compiler_params=pltpu.CompilerParams(
            collective_id=0, has_side_effects=True, vmem_limit_bytes=48 * 2**20
        ),
    )(*weights, norm_train.reshape(1, -1), norm_step.reshape(1, -1))
    pieces = []
    for i in [0, 7, 1, 2, 8, 9, 3, 4, 5, 6]:
        rows = out[i].shape[0]
        cut = rows // PIECES if i == 0 else rows
        pieces += [(i, r, cut) for r in range(0, rows, cut)]
    done = pl.pallas_call(
        functools.partial(write, pieces),
        out_shape=[jax.ShapeDtypeStruct(o.shape, o.dtype) for o in out],
        in_specs=[anywhere] * 10,
        out_specs=[anywhere] * 10,
        scratch_shapes=[dma((len(pieces),))],
        compiler_params=pltpu.CompilerParams(vmem_limit_bytes=2**20),
    )(*out)
    return tuple(d.reshape(-1) if 3 <= i <= 6 else d for i, d in enumerate(done))


def solution(mesh):
    n_rows, n_model = mesh.shape["rows"], mesh.shape["model"]

    def body(*arrays):
        share = arrays[0].shape[0]
        widths = [arrays[3 * a].shape[1] for a in range(3)]
        width = min(widths)
        d_model = share * n_rows
        fits = (
            n_rows % SIDE == 0
            and 2 <= n_rows // SIDE <= 4
            and share % TILE == 0
            and share > EARLY
            and width % 128 == 0
            and all(w % width == 0 for w in widths)
            and sum(widths) + width <= 2 * widths[0]
        )
        if not fits:
            return plain(d_model, arrays)
        blocks = tuple(
            (a, s, width) for a, w in enumerate(widths) for s in range(0, w, width)
        )
        return fused(n_rows, n_model, d_model, blocks, arrays)

    return jax.shard_map(
        body,
        mesh=mesh,
        in_specs=(P("rows", "model"),) * 9 + (P(("rows", "model")),) * 2,
        out_specs=(
            *(P(None, "model"),) * 3,
            *(P("model"),) * 3,
            P(),
            *(P("rows", "model"),) * 3,
        ),
        check_vma=False,
    )
```

```python
import functools

import jax
import jax.numpy as jnp
from jax import lax
from jax.experimental import pallas as pl
from jax.experimental.pallas import tpu as pltpu
from jax.sharding import PartitionSpec as P

learn_rate = 0.01
decay_rate = 0.05
tiny_value = 1e-08

MESH = pl.DeviceIdType.MESH
SIDE = 2
TILE = 32
EARLY = 128
PAIR = 1


def adam(w, first, second):
    return w - learn_rate * (first / (jnp.sqrt(second) + tiny_value) + decay_rate * w)


def plain(d_model, arrays):
    *weights, norm_train, norm_step = arrays
    results = [adam(*weights[3 * i : 3 * i + 3]) for i in range(3)]
    totals = lax.psum(tuple(jnp.sum(jnp.abs(r), axis=0) for r in results), "rows")
    columns = [t / d_model for t in totals]
    finals = [
        lax.all_gather((r / c).astype(jnp.bfloat16), "rows", axis=0, tiled=True)
        for r, c in zip(results, columns)
    ]
    serve = lax.all_gather(
        (norm_train + norm_step).astype(jnp.bfloat16), ("rows", "model"), axis=0, tiled=True
    )
    return (*finals, *columns, serve, *results)


def wait_bytes(ref, sem):
    pltpu.make_async_copy(ref, ref, sem).wait()


def on_core(work):
    core = lax.axis_index("model") % 2
    for c in range(2):
        pl.when(core == c)(functools.partial(work, c))


class Gather:
    def __init__(self, n_rows, share, width, count, skip, whole, own, sems):
        self.line, self.share, self.width = n_rows // SIDE, share, width
        self.count, self.skip, self.whole, self.own = count, skip, whole, own
        (self.own_send, self.up_send, self.down_send, self.side_send,
         self.line_recv, self.side_recv) = sems
        self.me = lax.axis_index("rows")
        self.z, self.y = self.me // SIDE, self.me % SIDE
        self.cut = cut_of(self.line, share, count)
        cut = self.cut
        self.chunks = [(j, 0, share, False) for j in range(count) if j != PAIR]
        self.chunks += [(PAIR, cut, share, False), (PAIR, 0, cut, False), (PAIR, 0, cut, True)]
        self.spread = len(self.chunks) - 2

    def part(self, slot, owner, first, last, ref=None):
        cols = pl.ds(slot * self.width, self.width)
        if ref is not None:
            return ref.at[pl.ds(first, last - first), cols]
        rows = pl.ds(pl.multiple_of(owner * self.share + first, 16), last - first)
        return self.whole.at[rows, cols]

    def some(self, rows):
        return self.whole.at[pl.ds(0, rows // 2), pl.ds(0, 2 * self.width)]

    def to_line(self, zs, c, up, to, near=False, mine=False):
        slot, first, last, crossed = self.chunks[c]
        if near and slot == 0:
            first = self.skip
        owner = zs * SIDE + (1 - self.y if crossed else self.y)
        there = self.part(slot, owner, first, last)
        here = there
        if mine and not crossed:
            here = self.part(slot, owner, first, last, self.own)
        send = self.own_send.at[int(up)] if mine else (self.up_send if up else self.down_send).at[zs]
        return pltpu.make_async_remote_copy(
            src_ref=here,
            dst_ref=there,
            send_sem=send,
            recv_sem=self.line_recv.at[jnp.where(zs < to, zs, zs - 1), c],
            device_id={"rows": self.me + (SIDE if up else -SIDE)},
            device_id_type=MESH,
        )

    def to_side(self, zs, slot, first, from_me=True, mine=False):
        owner = zs * SIDE + (self.y if from_me else 1 - self.y)
        there = self.part(slot, owner, first, self.share)
        here = self.part(slot, owner, first, self.share, self.own) if mine else there
        group = self.line if mine and slot == PAIR else zs
        return pltpu.make_async_remote_copy(
            src_ref=here,
            dst_ref=there,
            send_sem=self.side_send.at[group],
            recv_sem=self.side_recv.at[group],
            device_id={"rows": self.z * SIDE + 1 - self.y},
            device_id_type=MESH,
        )

    def both_ways(self, c):
        z = self.z

        @pl.when(z > 0)
        def _():
            self.to_line(z, c, False, z - 1, True, True).start()

        @pl.when(z < self.line - 1)
        def _():
            self.to_line(z, c, True, z + 1, True, True).start()

    def send_own(self, slot):
        for c, chunk in enumerate(self.chunks):
            if chunk[0] == slot and not chunk[3]:
                self.both_ways(c)
        self.to_side(self.z, slot, self.skip if slot == 0 else 0, mine=True).start()

    def relay(self):
        z, line = self.z, self.line
        self.to_side(z, PAIR, 0, False, True).wait_recv()
        self.both_ways(len(self.chunks) - 1)
        for d in range(1, line):
            for c, (slot, first, _, _) in enumerate(self.chunks):

                @pl.when(z - d >= 0)
                def _():
                    self.to_line(z - d, c, True, z, d == 1).wait_recv()

                    @pl.when(z < line - 1)
                    def _():
                        self.to_line(z - d, c, True, z + 1).start()

                    if c < self.spread:
                        self.to_side(z - d, slot, first).start()

                @pl.when(z + d < line)
                def _():
                    self.to_line(z + d, c, False, z, d == 1).wait_recv()

                    @pl.when(z > 0)
                    def _():
                        self.to_line(z + d, c, False, z - 1).start()

                    if c < self.spread:
                        self.to_side(z + d, slot, first).start()

    def finish(self):
        z, line, share, count, cut = self.z, self.line, self.share, self.count, self.cut
        full = count * share + cut

        @pl.when(z > 0)
        def _():
            wait_bytes(self.some(full - self.skip), self.own_send.at[0])

        @pl.when(z < line - 1)
        def _():
            wait_bytes(self.some(full - self.skip), self.own_send.at[1])

        self.to_side(z, PAIR, 0, mine=True).wait_send()
        for zs in range(line):

            @pl.when((z > 0) & (z < zs))
            def _():
                wait_bytes(self.some(full), self.down_send.at[zs])

            @pl.when((z < line - 1) & (z > zs))
            def _():
                wait_bytes(self.some(full), self.up_send.at[zs])

            for sem in (self.side_recv, self.side_send):

                @pl.when(z == zs)
                def _():
                    wait_bytes(self.some((count - 1) * share - self.skip), sem.at[zs])

                @pl.when(z != zs)
                def _():
                    wait_bytes(self.some(count * share - cut), sem.at[zs])


def cut_of(line, share, count):
    return max(32, round(count * share / (2 * (line - 1)) / 32) * 32)


def gather_sems(line, most):
    dma = pltpu.SemaphoreType.DMA
    return [dma((2,)), dma((line,)), dma((line,)), dma((line + 1,)),
            dma((line - 1, most + 2)), dma((line + 1,))]


def opening(n_rows, n_model, blocks, orders, d_model, *refs):
    ins, refs = refs[:9], refs[9:]
    nt_ref, ns_ref = refs[:2]
    whole, later, cols, norm_out, results = refs[2], refs[3], refs[4:7], refs[7], refs[8:11]
    bufs = refs[11:14]
    (norms, lines, sums, gains, in_sem, norm_sem, sum_send, sum_recv, gain_send, gain_recv,
     early, early_send, early_recv) = refs[14:27]
    sems = refs[27:]

    line = n_rows // SIDE
    me = lax.axis_index("rows")
    col = lax.axis_index("model")
    z, y = me // SIDE, me % SIDE
    other = 1 - y
    share = bufs[0].shape[1]
    width = blocks[0][2]

    def load(b):
        a, start, _ = blocks[b]
        where = (slice(None), pl.ds(start, width))
        for k in range(3):
            pltpu.make_async_copy(
                ins[3 * a + k].at[where], bufs[a].at[(k, *where)], in_sem.at[b]
            ).start()

    on_core(lambda c: load(orders[c][0][0]))
    barrier = pltpu.get_barrier_semaphore()
    for k in range(1, n_rows):
        pl.semaphore_signal(
            barrier, inc=1, device_id={"rows": lax.rem(me + k, n_rows)}, device_id_type=MESH
        )
    for k in range(1, n_model):
        pl.semaphore_signal(
            barrier, inc=1, device_id={"model": lax.rem(col + k, n_model)}, device_id_type=MESH
        )

    def step(b, rest=()):
        a, start, _ = blocks[b]
        wait_bytes(bufs[a].at[:, :, pl.ds(start, width)], in_sem.at[b])
        if rest:
            for r in rest:
                load(r)
            for n, ref in enumerate((nt_ref, ns_ref)):
                pltpu.make_async_copy(ref, norms.at[n], norm_sem.at[0]).start()

        def one(i, acc):
            rows = pl.ds(pl.multiple_of(i * TILE, TILE), TILE)
            where = (rows, pl.ds(start, width))
            r = adam(*(bufs[a][(k, *where)] for k in range(3)))
            results[a][where] = r
            m = jnp.abs(r).reshape(TILE // 8, 8, width)
            return acc + jnp.sum(m, axis=0)

        acc = lax.fori_loop(0, share // TILE, one, jnp.zeros((8, width), jnp.float32))
        sums[b, me] = jnp.sum(acc, axis=0, keepdims=True)

    def sum_copy(b, k):
        return pltpu.make_async_remote_copy(
            src_ref=sums.at[b, me],
            dst_ref=sums.at[b, me],
            send_sem=sum_send.at[0],
            recv_sem=sum_recv.at[b],
            device_id={"rows": lax.rem(me + k, n_rows)},
            device_id_type=MESH,
        )

    def early_copy(b, n, to):
        a, start, _ = blocks[b]
        return pltpu.make_async_remote_copy(
            src_ref=results[a].at[pl.ds(0, EARLY), pl.ds(start, width)],
            dst_ref=early.at[n],
            send_sem=early_send.at[n],
            recv_sem=early_recv.at[n],
            device_id={"rows": to},
            device_id_type=MESH,
        )

    def gain_model(k):
        return pltpu.make_async_remote_copy(
            src_ref=gains.at[me, col],
            dst_ref=gains.at[me, col],
            send_sem=gain_send.at[0],
            recv_sem=gain_recv.at[0],
            device_id={"model": lax.rem(col + k, n_model)},
            device_id_type=MESH,
        )

    def gain_rows(k):
        return pltpu.make_async_remote_copy(
            src_ref=gains.at[me],
            dst_ref=gains.at[me],
            send_sem=gain_send.at[1],
            recv_sem=gain_recv.at[1],
            device_id={"rows": lax.rem(me + k, n_rows)},
            device_id_type=MESH,
        )

    def work(core):
        now, then = orders[core]
        order = now + then
        gather = Gather(n_rows, share, width, len(now), EARLY, whole, None, sems)
        for i, b in enumerate(order):
            step(b, order[1:] if i == 0 else ())
            if i == 0:
                pl.semaphore_wait(barrier, n_rows + n_model - 2)
            for k in range(1, n_rows):
                sum_copy(b, k).start()
            if i == 0:
                early_copy(b, 0, z * SIDE + other).start()

                @pl.when(z < line - 1)
                def _():
                    early_copy(b, 1, me + SIDE).start()

                @pl.when(z > 0)
                def _():
                    early_copy(b, 2, me - SIDE).start()

        wait_bytes(norms, norm_sem.at[0])
        gains[me, col] = norms[0] + norms[1]
        for k in range(1, n_model):
            gain_model(k).start()

        for i, b in enumerate(order):
            a, start, _ = blocks[b]
            wait_bytes(sums.at[b, pl.ds(0, n_rows - 1)], sum_recv.at[b])
            total = sums[b, 0]
            for k in range(1, n_rows):
                total = total + sums[b, k]
            column = total / d_model
            cols[a][:, pl.ds(start, width)] = column
            scale = jnp.broadcast_to(1.0 / column, (TILE, width))
            mine = i < len(now)
            slot = i if mine else i - len(now)

            def one(t, carry):
                rows = pl.ds(pl.multiple_of(t * TILE, TILE), TILE)
                value = (results[a][rows, pl.ds(start, width)] * scale).astype(jnp.bfloat16)
                where = pl.ds(slot * width, width)
                if mine:
                    whole[pl.ds(pl.multiple_of(me * share + t * TILE, TILE), TILE), where] = value
                else:
                    later[rows, where] = value
                return carry

            lax.fori_loop(0, share // TILE, one, 0)
            if mine:
                gather.send_own(slot)

        a, start, _ = blocks[order[0]]
        scale = jnp.broadcast_to(1.0 / cols[a][:, pl.ds(start, width)], (TILE, width))

        def scaled(n, owner):
            early_copy(order[0], n, owner).wait_recv()

            def one(t, carry):
                rows = pl.ds(pl.multiple_of(t * TILE, TILE), TILE)
                there = pl.ds(pl.multiple_of(owner * share + t * TILE, TILE), TILE)
                whole[there, pl.ds(0, width)] = (early[n, rows] * scale).astype(jnp.bfloat16)
                return carry

            lax.fori_loop(0, EARLY // TILE, one, 0)

        @pl.when(z > 0)
        def _():
            scaled(1, me - SIDE)

        @pl.when(z < line - 1)
        def _():
            scaled(2, me + SIDE)

        scaled(0, z * SIDE + other)

        wait_bytes(gains.at[0, pl.ds(0, n_model - 1)], gain_recv.at[0])
        for k in range(1, n_rows):
            gain_rows(k).start()
        gather.relay()
        early_copy(order[0], 0, me).wait_send()

        @pl.when(z < line - 1)
        def _():
            early_copy(order[0], 1, me).wait_send()

        @pl.when(z > 0)
        def _():
            early_copy(order[0], 2, me).wait_send()

        gather.finish()

    on_core(work)
    wait_bytes(gains.at[pl.ds(0, n_rows - 1)], gain_recv.at[1])
    for r in range(n_rows):
        for m in range(n_model):
            lines[pl.ds(r * n_model + m, 1), :] = gains[r, m]
    norm_out[...] = lines[...].astype(jnp.bfloat16)
    wait_bytes(gains.at[0, pl.ds(0, n_model - 1)], gain_send.at[0])
    wait_bytes(gains.at[pl.ds(0, n_rows - 1)], gain_send.at[1])
    wait_bytes(sums.at[:, pl.ds(0, n_rows - 1)], sum_send.at[0])


def closing(n_rows, blocks, orders, own, token, whole, *sems):
    line = n_rows // SIDE
    me = lax.axis_index("rows")
    z, y = me // SIDE, me % SIDE
    share, width = own.shape[0], blocks[0][2]
    barrier = pltpu.get_barrier_semaphore()

    def signal(who):
        pl.semaphore_signal(barrier, inc=1, device_id={"rows": who}, device_id_type=MESH)

    signal(z * SIDE + 1 - y)

    @pl.when(z > 0)
    def _():
        signal(me - SIDE)

    @pl.when(z < line - 1)
    def _():
        signal(me + SIDE)

    pl.semaphore_wait(barrier, 1 + jnp.where(z > 0, 1, 0) + jnp.where(z < line - 1, 1, 0))

    def work(core):
        count = len(orders[core][1])
        gather = Gather(n_rows, share, width, count, 0, whole, own, sems)
        for slot in range(count):
            gather.send_own(slot)

        def one(t, carry):
            rows = pl.ds(pl.multiple_of(t * TILE, TILE), TILE)
            there = pl.ds(pl.multiple_of(me * share + t * TILE, TILE), TILE)
            whole[there, pl.ds(0, count * width)] = own[rows, pl.ds(0, count * width)]
            return carry

        lax.fori_loop(0, share // TILE, one, 0)
        gather.relay()
        gather.finish()

    on_core(work)


def put(blocks, orders, phase, whole, finals, sem):
    def work(core):
        copies = []
        for slot, b in enumerate(orders[core][phase]):
            a, start, width = blocks[b]
            c = pltpu.make_async_copy(
                whole.at[:, pl.ds(slot * width, width)],
                finals[a].at[:, pl.ds(start, width)],
                sem.at[slot],
            )
            c.start()
            copies.append(c)
        for c in copies:
            c.wait()

    on_core(work)


def write(blocks, orders, *refs):
    whole, small, finals, outs, token, sem = refs[0], refs[1:8], refs[8:11], refs[11:18], refs[18], refs[19]
    most = max(len(o) for c in orders for o in c)
    copies = []
    for n, (src, dst) in enumerate(zip(small, outs)):
        c = pltpu.make_async_copy(src, dst, sem.at[most + n])
        c.start()
        copies.append(c)
    token[...] = jnp.zeros_like(token)
    put(blocks, orders, 0, whole, finals, sem)
    for c in copies:
        c.wait()


def rest(blocks, orders, whole, *refs):
    put(blocks, orders, 1, whole, refs[3:6], refs[6])


def fused(n_rows, n_model, d_model, blocks, arrays):
    *weights, norm_train, norm_step = arrays
    share = weights[0].shape[0]
    widths = [weights[3 * a].shape[1] for a in range(3)]
    line, nb, width = n_rows // SIDE, len(blocks), blocks[0][2]
    unit = norm_train.shape[0]
    big = [b for b in range(nb) if blocks[b][0] == 0]
    few = [b for b in range(nb) if blocks[b][0] != 0]
    orders = ((big, few), (few, big))
    most = max(len(big), len(few))
    anywhere = pl.BlockSpec(memory_space=pl.ANY)
    vmem = pl.BlockSpec(memory_space=pltpu.VMEM)
    f32, b16, dma = jnp.float32, jnp.bfloat16, pltpu.SemaphoreType.DMA
    whole, own, *small = pl.pallas_call(
        functools.partial(opening, n_rows, n_model, blocks, orders, d_model),
        out_shape=[
            pltpu.VMEM((d_model, most * width), b16),
            pltpu.VMEM((share, most * width), b16),
            *(pltpu.VMEM((1, w), f32) for w in widths),
            pltpu.VMEM((n_rows * n_model, unit), b16),
            *(pltpu.VMEM((share, w), f32) for w in widths),
        ],
        in_specs=[anywhere] * 11,
        out_specs=[vmem] * 9,
        scratch_shapes=[
            *(pltpu.VMEM((3, share, w), f32) for w in widths),
            pltpu.VMEM((2, 1, unit), f32),
            pltpu.VMEM((n_rows * n_model, unit), f32),
            pltpu.VMEM((nb, n_rows, 1, width), f32),
            pltpu.VMEM((n_rows, n_model, 1, unit), f32),
            dma((nb,)),
            dma((1,)),
            dma((1,)),
            dma((nb,)),
            dma((2,)),
            dma((2,)),
            pltpu.VMEM((3, EARLY, width), f32),
            dma((3,)),
            dma((3,)),
            *gather_sems(line, most),
        ],
        compiler_params=pltpu.CompilerParams(
            collective_id=0, has_side_effects=True, vmem_limit_bytes=50 * 2**20
        ),
    )(*weights, norm_train.reshape(1, -1), norm_step.reshape(1, -1))
    *finals, c0, c1, c2, serve, r0, r1, r2, token = pl.pallas_call(
        functools.partial(write, blocks, orders),
        out_shape=[
            *(jax.ShapeDtypeStruct((d_model, w), b16) for w in widths),
            *(jax.ShapeDtypeStruct(o.shape, o.dtype) for o in small),
            pltpu.VMEM((8, 128), f32),
        ],
        in_specs=[anywhere] * 8,
        out_specs=[anywhere] * 10 + [vmem],
        scratch_shapes=[dma((most + 7,))],
        compiler_params=pltpu.CompilerParams(vmem_limit_bytes=2**20),
    )(whole, *small)
    whole = pl.pallas_call(
        functools.partial(closing, n_rows, blocks, orders),
        out_shape=pltpu.VMEM((d_model, most * width), b16),
        in_specs=[vmem, anywhere],
        out_specs=vmem,
        scratch_shapes=gather_sems(line, most),
        compiler_params=pltpu.CompilerParams(
            collective_id=1, has_side_effects=True, vmem_limit_bytes=40 * 2**20
        ),
    )(own, token)
    finals = pl.pallas_call(
        functools.partial(rest, blocks, orders),
        out_shape=[jax.ShapeDtypeStruct((d_model, w), b16) for w in widths],
        in_specs=[anywhere] * 4,
        out_specs=[anywhere] * 3,
        scratch_shapes=[dma((most,))],
        input_output_aliases={1: 0, 2: 1, 3: 2},
        compiler_params=pltpu.CompilerParams(vmem_limit_bytes=2**20),
    )(whole, *finals)
    return (*finals, *(d.reshape(-1) for d in (c0, c1, c2, serve)), r0, r1, r2)


def solution(mesh):
    n_rows, n_model = mesh.shape["rows"], mesh.shape["model"]

    def body(*arrays):
        share = arrays[0].shape[0]
        widths = [arrays[3 * a].shape[1] for a in range(3)]
        width = min(widths)
        d_model = share * n_rows
        line = n_rows // SIDE
        counts = (widths[0] // width, (widths[1] + widths[2]) // width)
        fits = (
            n_rows % SIDE == 0
            and n_model % 2 == 0
            and 2 <= line <= 4
            and share % TILE == 0
            and share > EARLY
            and width % 128 == 0
            and all(w % width == 0 for w in widths)
            and all(2 <= c <= 6 and cut_of(line, share, c) < share for c in counts)
        )
        if not fits:
            return plain(d_model, arrays)
        blocks = tuple(
            (a, s, width) for a, w in enumerate(widths) for s in range(0, w, width)
        )
        return fused(n_rows, n_model, d_model, blocks, arrays)

    return jax.shard_map(
        body,
        mesh=mesh,
        in_specs=(P("rows", "model"),) * 9 + (P(("rows", "model")),) * 2,
        out_specs=(
            *(P(None, "model"),) * 3,
            *(P("model"),) * 3,
            P(),
            *(P("rows", "model"),) * 3,
        ),
        check_vma=False,
    )
```

```python
import functools

import jax
import jax.numpy as jnp
from jax import lax
from jax.experimental import pallas as pl
from jax.experimental.pallas import tpu as pltpu
from jax.sharding import PartitionSpec as P

learn_rate = 0.01
decay_rate = 0.05
tiny_value = 1e-08

MESH = pl.DeviceIdType.MESH
SIDE = 2
TILE = 32
EARLY = (128, 128)


def adam(w, first, second):
    return w - learn_rate * (first / (jnp.sqrt(second) + tiny_value) + decay_rate * w)


def plain(d_model, arrays):
    *weights, norm_train, norm_step = arrays
    results = [adam(*weights[3 * i : 3 * i + 3]) for i in range(3)]
    totals = lax.psum(tuple(jnp.sum(jnp.abs(r), axis=0) for r in results), "rows")
    columns = [t / d_model for t in totals]
    finals = [
        lax.all_gather((r / c).astype(jnp.bfloat16), "rows", axis=0, tiled=True)
        for r, c in zip(results, columns)
    ]
    serve = lax.all_gather(
        (norm_train + norm_step).astype(jnp.bfloat16), ("rows", "model"), axis=0, tiled=True
    )
    return (*finals, *columns, serve, *results)


def wait_bytes(ref, sem):
    pltpu.make_async_copy(ref, ref, sem).wait()


def on_core(work):
    core = lax.axis_index("model") % 2
    for c in range(2):
        pl.when(core == c)(functools.partial(work, c))


class Gather:
    def __init__(self, n_rows, share, width, count, skip, whole, own, sems):
        self.line, self.share, self.width = n_rows // SIDE, share, width
        self.count, self.skip, self.whole, self.own = count, skip, whole, own
        (self.own_send, self.up_send, self.down_send, self.side_send,
         self.line_recv, self.side_recv) = sems
        self.me = lax.axis_index("rows")
        self.z, self.y = self.me // SIDE, self.me % SIDE
        self.cut = cut_of(self.line, share, count)
        cut = self.cut
        self.pair = pair = min(1, count - 1)
        full = [(j, 0, share, False) for j in range(count) if j != pair]
        head = [(pair, cut, share, False)]
        if own is not None:
            slot, first, last, _ = (full or head).pop()
            mid = (first + last) // 64 * 32
            head += [(slot, first, mid, False), (slot, mid, last, False)]
        self.chunks = full + head + [(pair, 0, cut, False), (pair, 0, cut, True)]
        self.spread = len(self.chunks) - 2

    def part(self, slot, owner, first, last, ref=None):
        cols = pl.ds(slot * self.width, self.width)
        if ref is not None:
            return ref.at[pl.ds(first, last - first), cols]
        rows = pl.ds(pl.multiple_of(owner * self.share + first, 16), last - first)
        return self.whole.at[rows, cols]

    def some(self, rows):
        return self.whole.at[pl.ds(0, rows // 2), pl.ds(0, 2 * self.width)]

    def to_line(self, zs, c, up, to, near=False, mine=False):
        slot, first, last, crossed = self.chunks[c]
        if near and slot == 0:
            first = max(first, self.skip)
        owner = zs * SIDE + (1 - self.y if crossed else self.y)
        there = self.part(slot, owner, first, last)
        here = there
        if mine and not crossed:
            here = self.part(slot, owner, first, last, self.own)
        send = self.own_send.at[int(up)] if mine else (self.up_send if up else self.down_send).at[zs]
        return pltpu.make_async_remote_copy(
            src_ref=here,
            dst_ref=there,
            send_sem=send,
            recv_sem=self.line_recv.at[jnp.where(zs < to, zs, zs - 1), c],
            device_id={"rows": self.me + (SIDE if up else -SIDE)},
            device_id_type=MESH,
        )

    def to_side(self, zs, slot, first, from_me=True, mine=False, last=None):
        owner = zs * SIDE + (self.y if from_me else 1 - self.y)
        last = self.share if last is None else last
        there = self.part(slot, owner, first, last)
        here = self.part(slot, owner, first, last, self.own) if mine else there
        group = self.line if mine and slot == self.pair else zs
        return pltpu.make_async_remote_copy(
            src_ref=here,
            dst_ref=there,
            send_sem=self.side_send.at[group],
            recv_sem=self.side_recv.at[group],
            device_id={"rows": self.z * SIDE + 1 - self.y},
            device_id_type=MESH,
        )

    def both_ways(self, c):
        z = self.z

        @pl.when(z > 0)
        def _():
            self.to_line(z, c, False, z - 1, True, True).start()

        @pl.when(z < self.line - 1)
        def _():
            self.to_line(z, c, True, z + 1, True, True).start()

    def send_own(self, slot):
        for c, chunk in enumerate(self.chunks):
            if chunk[0] == slot and not chunk[3]:
                self.both_ways(c)
        self.to_side(self.z, slot, self.skip if slot == 0 else 0, mine=True).start()

    def pass_on(self, d, c):
        z, line = self.z, self.line
        slot, first, last, _ = self.chunks[c]

        @pl.when(z - d >= 0)
        def _():
            self.to_line(z - d, c, True, z, d == 1).wait_recv()

            @pl.when(z < line - 1)
            def _():
                self.to_line(z - d, c, True, z + 1).start()

            if c < self.spread:
                self.to_side(z - d, slot, first, last=last).start()

        @pl.when(z + d < line)
        def _():
            self.to_line(z + d, c, False, z, d == 1).wait_recv()

            @pl.when(z > 0)
            def _():
                self.to_line(z + d, c, False, z - 1).start()

            if c < self.spread:
                self.to_side(z + d, slot, first, last=last).start()

    def relay(self):
        crossed = len(self.chunks) - 1
        for d in range(1, self.line):
            for c in range(crossed):
                self.pass_on(d, c)
            if d == 1:
                self.to_side(self.z, self.pair, 0, False, True).wait_recv()
                self.both_ways(crossed)
        for d in range(1, self.line):
            self.pass_on(d, crossed)

    def finish(self):
        z, line, share, count, cut = self.z, self.line, self.share, self.count, self.cut
        full = count * share + cut

        @pl.when(z > 0)
        def _():
            wait_bytes(self.some(full - self.skip), self.own_send.at[0])

        @pl.when(z < line - 1)
        def _():
            wait_bytes(self.some(full - self.skip), self.own_send.at[1])

        self.to_side(z, self.pair, 0, mine=True).wait_send()
        for zs in range(line):

            @pl.when((z > 0) & (z < zs))
            def _():
                wait_bytes(self.some(full), self.down_send.at[zs])

            @pl.when((z < line - 1) & (z > zs))
            def _():
                wait_bytes(self.some(full), self.up_send.at[zs])

            for sem in (self.side_recv, self.side_send):

                if count > 1:

                    @pl.when(z == zs)
                    def _():
                        wait_bytes(self.some((count - 1) * share - self.skip), sem.at[zs])

                @pl.when(z != zs)
                def _():
                    wait_bytes(self.some(count * share - cut), sem.at[zs])


def cut_of(line, share, count):
    return max(32, round(count * share / (2 * (line - 1)) / 32) * 32)


def gather_sems(line, most):
    dma = pltpu.SemaphoreType.DMA
    return [dma((2,)), dma((line,)), dma((line,)), dma((line + 1,)),
            dma((line - 1, most + 3)), dma((line + 1,))]


def opening(n_rows, n_model, blocks, orders, d_model, *refs):
    ins, refs = refs[:9], refs[9:]
    nt_ref, ns_ref = refs[:2]
    whole, later, cols, norm_out, results = refs[2], refs[3], refs[4:7], refs[7], refs[8:11]
    bufs = refs[11:14]
    (norms, lines, sums, gains, in_sem, norm_sem, sum_send, sum_recv, gain_send, gain_recv,
     early, early_send, early_recv) = refs[14:27]
    sems = refs[27:]

    line = n_rows // SIDE
    me = lax.axis_index("rows")
    col = lax.axis_index("model")
    z, y = me // SIDE, me % SIDE
    other = 1 - y
    share = bufs[0].shape[1]
    width = blocks[0][2]

    def load(b):
        a, start, _ = blocks[b]
        where = (slice(None), pl.ds(start, width))
        for k in range(3):
            pltpu.make_async_copy(
                ins[3 * a + k].at[where], bufs[a].at[(k, *where)], in_sem.at[b]
            ).start()

    on_core(lambda c: load(orders[c][0][0]))
    barrier = pltpu.get_barrier_semaphore()
    for k in range(1, n_rows):
        pl.semaphore_signal(
            barrier, inc=1, device_id={"rows": lax.rem(me + k, n_rows)}, device_id_type=MESH
        )
    for k in range(1, n_model):
        pl.semaphore_signal(
            barrier, inc=1, device_id={"model": lax.rem(col + k, n_model)}, device_id_type=MESH
        )

    def step(b, rest=()):
        a, start, _ = blocks[b]
        wait_bytes(bufs[a].at[:, :, pl.ds(start, width)], in_sem.at[b])
        if rest:
            for r in rest:
                load(r)
            for n, ref in enumerate((nt_ref, ns_ref)):
                pltpu.make_async_copy(ref, norms.at[n], norm_sem.at[0]).start()

        def one(i, acc):
            rows = pl.ds(pl.multiple_of(i * TILE, TILE), TILE)
            where = (rows, pl.ds(start, width))
            r = adam(*(bufs[a][(k, *where)] for k in range(3)))
            results[a][where] = r
            m = jnp.abs(r).reshape(TILE // 8, 8, width)
            return acc + jnp.sum(m, axis=0)

        acc = lax.fori_loop(0, share // TILE, one, jnp.zeros((8, width), jnp.float32))
        sums[b, me] = jnp.sum(acc, axis=0, keepdims=True)

    def sum_copy(b, k):
        return pltpu.make_async_remote_copy(
            src_ref=sums.at[b, me],
            dst_ref=sums.at[b, me],
            send_sem=sum_send.at[0],
            recv_sem=sum_recv.at[b],
            device_id={"rows": lax.rem(me + k, n_rows)},
            device_id_type=MESH,
        )

    def early_copy(b, n, to, rows):
        a, start, _ = blocks[b]
        return pltpu.make_async_remote_copy(
            src_ref=results[a].at[pl.ds(0, rows), pl.ds(start, width)],
            dst_ref=early.at[n, pl.ds(0, rows)],
            send_sem=early_send.at[n],
            recv_sem=early_recv.at[n],
            device_id={"rows": to},
            device_id_type=MESH,
        )

    def gain_model(k):
        return pltpu.make_async_remote_copy(
            src_ref=gains.at[me, col],
            dst_ref=gains.at[me, col],
            send_sem=gain_send.at[0],
            recv_sem=gain_recv.at[0],
            device_id={"model": lax.rem(col + k, n_model)},
            device_id_type=MESH,
        )

    def gain_rows(k):
        return pltpu.make_async_remote_copy(
            src_ref=gains.at[me],
            dst_ref=gains.at[me],
            send_sem=gain_send.at[1],
            recv_sem=gain_recv.at[1],
            device_id={"rows": lax.rem(me + k, n_rows)},
            device_id_type=MESH,
        )

    def work(core):
        now, then = orders[core]
        order = now + then
        ahead = EARLY[core]
        gather = Gather(n_rows, share, width, len(now), ahead, whole, None, sems)
        for i, b in enumerate(order):
            step(b, order[1:] if i == 0 else ())
            if i == 0:
                pl.semaphore_wait(barrier, n_rows + n_model - 2)
            for k in range(1, n_rows):
                sum_copy(b, k).start()
            if i == 0 and ahead:
                early_copy(b, 0, z * SIDE + other, ahead).start()

                @pl.when(z < line - 1)
                def _():
                    early_copy(b, 1, me + SIDE, ahead).start()

                @pl.when(z > 0)
                def _():
                    early_copy(b, 2, me - SIDE, ahead).start()

        wait_bytes(norms, norm_sem.at[0])
        gains[me, col] = norms[0] + norms[1]
        for k in range(1, n_model):
            gain_model(k).start()

        for i, b in enumerate(order):
            a, start, _ = blocks[b]
            wait_bytes(sums.at[b, pl.ds(0, n_rows - 1)], sum_recv.at[b])
            total = sums[b, 0]
            for k in range(1, n_rows):
                total = total + sums[b, k]
            column = total / d_model
            cols[a][:, pl.ds(start, width)] = column
            scale = jnp.broadcast_to(1.0 / column, (TILE, width))
            mine = i < len(now)
            slot = i if mine else i - len(now)

            def one(t, carry):
                rows = pl.ds(pl.multiple_of(t * TILE, TILE), TILE)
                value = (results[a][rows, pl.ds(start, width)] * scale).astype(jnp.bfloat16)
                where = pl.ds(slot * width, width)
                if mine:
                    whole[pl.ds(pl.multiple_of(me * share + t * TILE, TILE), TILE), where] = value
                else:
                    later[rows, where] = value
                return carry

            lax.fori_loop(0, share // TILE, one, 0)
            if mine:
                gather.send_own(slot)

        if ahead:
            a, start, _ = blocks[order[0]]
            scale = jnp.broadcast_to(1.0 / cols[a][:, pl.ds(start, width)], (TILE, width))

            def scaled(n, owner):
                early_copy(order[0], n, owner, ahead).wait_recv()

                def one(t, carry):
                    rows = pl.ds(pl.multiple_of(t * TILE, TILE), TILE)
                    there = pl.ds(pl.multiple_of(owner * share + t * TILE, TILE), TILE)
                    whole[there, pl.ds(0, width)] = (early[n, rows] * scale).astype(jnp.bfloat16)
                    return carry

                lax.fori_loop(0, ahead // TILE, one, 0)

            @pl.when(z > 0)
            def _():
                scaled(1, me - SIDE)

            @pl.when(z < line - 1)
            def _():
                scaled(2, me + SIDE)

            scaled(0, z * SIDE + other)

        wait_bytes(gains.at[0, pl.ds(0, n_model - 1)], gain_recv.at[0])
        for k in range(1, n_rows):
            gain_rows(k).start()
        gather.relay()
        if ahead:
            early_copy(order[0], 0, me, ahead).wait_send()

            @pl.when(z < line - 1)
            def _():
                early_copy(order[0], 1, me, ahead).wait_send()

            @pl.when(z > 0)
            def _():
                early_copy(order[0], 2, me, ahead).wait_send()

        gather.finish()

    on_core(work)
    wait_bytes(gains.at[pl.ds(0, n_rows - 1)], gain_recv.at[1])
    for r in range(n_rows):
        for m in range(n_model):
            lines[pl.ds(r * n_model + m, 1), :] = gains[r, m]
    norm_out[...] = lines[...].astype(jnp.bfloat16)
    wait_bytes(gains.at[0, pl.ds(0, n_model - 1)], gain_send.at[0])
    wait_bytes(gains.at[pl.ds(0, n_rows - 1)], gain_send.at[1])
    wait_bytes(sums.at[:, pl.ds(0, n_rows - 1)], sum_send.at[0])


def closing(n_rows, blocks, orders, own, token, whole, *sems):
    line = n_rows // SIDE
    me = lax.axis_index("rows")
    z, y = me // SIDE, me % SIDE
    share, width = own.shape[0], blocks[0][2]
    barrier = pltpu.get_barrier_semaphore()

    def signal(who):
        pl.semaphore_signal(barrier, inc=1, device_id={"rows": who}, device_id_type=MESH)

    signal(z * SIDE + 1 - y)

    @pl.when(z > 0)
    def _():
        signal(me - SIDE)

    @pl.when(z < line - 1)
    def _():
        signal(me + SIDE)

    pl.semaphore_wait(barrier, 1 + jnp.where(z > 0, 1, 0) + jnp.where(z < line - 1, 1, 0))

    def work(core):
        count = len(orders[core][1])
        gather = Gather(n_rows, share, width, count, 0, whole, own, sems)
        for slot in range(count):
            gather.send_own(slot)

        def one(t, carry):
            rows = pl.ds(pl.multiple_of(t * TILE, TILE), TILE)
            there = pl.ds(pl.multiple_of(me * share + t * TILE, TILE), TILE)
            whole[there, pl.ds(0, count * width)] = own[rows, pl.ds(0, count * width)]
            return carry

        lax.fori_loop(0, share // TILE, one, 0)
        gather.relay()
        gather.finish()

    on_core(work)


def put(blocks, orders, phase, whole, finals, sem):
    def work(core):
        copies = []
        for slot, b in enumerate(orders[core][phase]):
            a, start, width = blocks[b]
            c = pltpu.make_async_copy(
                whole.at[:, pl.ds(slot * width, width)],
                finals[a].at[:, pl.ds(start, width)],
                sem.at[slot],
            )
            c.start()
            copies.append(c)
        for c in copies:
            c.wait()

    on_core(work)


def write(blocks, orders, *refs):
    whole, small, finals, outs, token, sem = refs[0], refs[1:8], refs[8:11], refs[11:18], refs[18], refs[19]
    most = max(len(o) for c in orders for o in c)
    copies = []
    for n, (src, dst) in enumerate(zip(small, outs)):
        c = pltpu.make_async_copy(src, dst, sem.at[most + n])
        c.start()
        copies.append(c)
    token[...] = jnp.zeros_like(token)
    put(blocks, orders, 0, whole, finals, sem)
    for c in copies:
        c.wait()


def rest(blocks, orders, whole, *refs):
    put(blocks, orders, 1, whole, refs[3:6], refs[6])


def fused(n_rows, n_model, d_model, blocks, arrays):
    *weights, norm_train, norm_step = arrays
    share = weights[0].shape[0]
    widths = [weights[3 * a].shape[1] for a in range(3)]
    line, nb, width = n_rows // SIDE, len(blocks), blocks[0][2]
    unit = norm_train.shape[0]
    big = [b for b in range(nb) if blocks[b][0] == 0]
    few = [b for b in range(nb) if blocks[b][0] != 0]
    orders = ((big, few), (few, big))
    most = [max(len(orders[c][p]) for c in range(2)) for p in range(2)]
    anywhere = pl.BlockSpec(memory_space=pl.ANY)
    vmem = pl.BlockSpec(memory_space=pltpu.VMEM)
    f32, b16, dma = jnp.float32, jnp.bfloat16, pltpu.SemaphoreType.DMA
    whole, own, *small = pl.pallas_call(
        functools.partial(opening, n_rows, n_model, blocks, orders, d_model),
        out_shape=[
            pltpu.VMEM((d_model, most[0] * width), b16),
            pltpu.VMEM((share, most[1] * width), b16),
            *(pltpu.VMEM((1, w), f32) for w in widths),
            pltpu.VMEM((n_rows * n_model, unit), b16),
            *(pltpu.VMEM((share, w), f32) for w in widths),
        ],
        in_specs=[anywhere] * 11,
        out_specs=[vmem] * 9,
        scratch_shapes=[
            *(pltpu.VMEM((3, share, w), f32) for w in widths),
            pltpu.VMEM((2, 1, unit), f32),
            pltpu.VMEM((n_rows * n_model, unit), f32),
            pltpu.VMEM((nb, n_rows, 1, width), f32),
            pltpu.VMEM((n_rows, n_model, 1, unit), f32),
            dma((nb,)),
            dma((1,)),
            dma((1,)),
            dma((nb,)),
            dma((2,)),
            dma((2,)),
            pltpu.VMEM((3, max(EARLY), width), f32),
            dma((3,)),
            dma((3,)),
            *gather_sems(line, most[0]),
        ],
        compiler_params=pltpu.CompilerParams(
            collective_id=0, has_side_effects=True, vmem_limit_bytes=49 * 2**20
        ),
    )(*weights, norm_train.reshape(1, -1), norm_step.reshape(1, -1))
    *finals, c0, c1, c2, serve, r0, r1, r2, token = pl.pallas_call(
        functools.partial(write, blocks, orders),
        out_shape=[
            *(jax.ShapeDtypeStruct((d_model, w), b16) for w in widths),
            *(jax.ShapeDtypeStruct(o.shape, o.dtype) for o in small),
            pltpu.VMEM((8, 128), f32),
        ],
        in_specs=[anywhere] * 8,
        out_specs=[anywhere] * 10 + [vmem],
        scratch_shapes=[dma((max(most) + 7,))],
        compiler_params=pltpu.CompilerParams(vmem_limit_bytes=2**20),
    )(whole, *small)
    whole = pl.pallas_call(
        functools.partial(closing, n_rows, blocks, orders),
        out_shape=pltpu.VMEM((d_model, most[1] * width), b16),
        in_specs=[vmem, anywhere],
        out_specs=vmem,
        scratch_shapes=gather_sems(line, most[1]),
        compiler_params=pltpu.CompilerParams(
            collective_id=1, has_side_effects=True, vmem_limit_bytes=40 * 2**20
        ),
    )(own, token)
    finals = pl.pallas_call(
        functools.partial(rest, blocks, orders),
        out_shape=[jax.ShapeDtypeStruct((d_model, w), b16) for w in widths],
        in_specs=[anywhere] * 4,
        out_specs=[anywhere] * 3,
        scratch_shapes=[dma((most[1],))],
        input_output_aliases={1: 0, 2: 1, 3: 2},
        compiler_params=pltpu.CompilerParams(vmem_limit_bytes=2**20),
    )(whole, *finals)
    return (*finals, *(d.reshape(-1) for d in (c0, c1, c2, serve)), r0, r1, r2)


def solution(mesh):
    n_rows, n_model = mesh.shape["rows"], mesh.shape["model"]

    def body(*arrays):
        share = arrays[0].shape[0]
        widths = [arrays[3 * a].shape[1] for a in range(3)]
        width = min(widths)
        d_model = share * n_rows
        line = n_rows // SIDE
        counts = (1, widths[0] // width, (widths[0] + widths[1] + widths[2]) // width - 1)
        fits = (
            n_rows % SIDE == 0
            and n_model % 2 == 0
            and 2 <= line <= 4
            and share % (2 * TILE) == 0
            and share > max(EARLY)
            and width % 128 == 0
            and all(w % width == 0 for w in widths)
            and counts[1] > 1
            and all(cut_of(line, share, c) <= share - 64 for c in counts)
        )
        if not fits:
            return plain(d_model, arrays)
        blocks = tuple(
            (a, s, width) for a, w in enumerate(widths) for s in range(0, w, width)
        )
        return fused(n_rows, n_model, d_model, blocks, arrays)

    return jax.shard_map(
        body,
        mesh=mesh,
        in_specs=(P("rows", "model"),) * 9 + (P(("rows", "model")),) * 2,
        out_specs=(
            *(P(None, "model"),) * 3,
            *(P("model"),) * 3,
            P(),
            *(P("rows", "model"),) * 3,
        ),
        check_vma=False,
    )
```

```python
import functools

import jax
import jax.numpy as jnp
from jax import lax
from jax.experimental import pallas as pl
from jax.experimental.pallas import tpu as pltpu
from jax.sharding import PartitionSpec as P

learn_rate = 0.01
decay_rate = 0.05
tiny_value = 1e-08

MESH = pl.DeviceIdType.MESH
SIDE = 2
TILE = 32
EARLY = (128, 128)


def adam(w, first, second):
    return w - learn_rate * (first / (jnp.sqrt(second) + tiny_value) + decay_rate * w)


def plain(d_model, arrays):
    *weights, norm_train, norm_step = arrays
    results = [adam(*weights[3 * i : 3 * i + 3]) for i in range(3)]
    totals = lax.psum(tuple(jnp.sum(jnp.abs(r), axis=0) for r in results), "rows")
    columns = [t / d_model for t in totals]
    finals = [
        lax.all_gather((r / c).astype(jnp.bfloat16), "rows", axis=0, tiled=True)
        for r, c in zip(results, columns)
    ]
    serve = lax.all_gather(
        (norm_train + norm_step).astype(jnp.bfloat16), ("rows", "model"), axis=0, tiled=True
    )
    return (*finals, *columns, serve, *results)


def wait_bytes(ref, sem):
    pltpu.make_async_copy(ref, ref, sem).wait()


def on_core(work):
    core = lax.axis_index("model") % 2
    for c in range(2):
        pl.when(core == c)(functools.partial(work, c))


class Gather:
    def __init__(self, n_rows, share, width, count, skip, whole, own, sems):
        self.line, self.share, self.width = n_rows // SIDE, share, width
        self.count, self.skip, self.whole, self.own = count, skip, whole, own
        (self.own_send, self.up_send, self.down_send, self.side_send,
         self.line_recv, self.side_recv) = sems
        self.me = lax.axis_index("rows")
        self.z, self.y = self.me // SIDE, self.me % SIDE
        self.cut = cut_of(self.line, share, count)
        cut = self.cut
        self.pair = pair = min(1, count - 1)
        full = [(j, 0, share, False) for j in range(count) if j != pair]
        head = [(pair, cut, share, False)]
        if own is not None:
            slot, first, last, _ = (full or head).pop()
            mid = (first + last) // 64 * 32
            head += [(slot, first, mid, False), (slot, mid, last, False)]
        self.chunks = full + head + [(pair, 0, cut, False), (pair, 0, cut, True)]
        self.spread = len(self.chunks) - 2

    def part(self, slot, owner, first, last, ref=None):
        cols = pl.ds(slot * self.width, self.width)
        if ref is not None:
            return ref.at[pl.ds(first, last - first), cols]
        rows = pl.ds(pl.multiple_of(owner * self.share + first, 16), last - first)
        return self.whole.at[rows, cols]

    def some(self, rows):
        return self.whole.at[pl.ds(0, rows // 2), pl.ds(0, 2 * self.width)]

    def to_line(self, zs, c, up, to, near=False, mine=False):
        slot, first, last, crossed = self.chunks[c]
        if near and slot == 0:
            first = max(first, self.skip)
        owner = zs * SIDE + (1 - self.y if crossed else self.y)
        there = self.part(slot, owner, first, last)
        here = there
        if mine and not crossed:
            here = self.part(slot, owner, first, last, self.own)
        send = self.own_send.at[int(up)] if mine else (self.up_send if up else self.down_send).at[zs]
        return pltpu.make_async_remote_copy(
            src_ref=here,
            dst_ref=there,
            send_sem=send,
            recv_sem=self.line_recv.at[jnp.where(zs < to, zs, zs - 1), c],
            device_id={"rows": self.me + (SIDE if up else -SIDE)},
            device_id_type=MESH,
        )

    def to_side(self, zs, slot, first, from_me=True, mine=False, last=None):
        owner = zs * SIDE + (self.y if from_me else 1 - self.y)
        last = self.share if last is None else last
        there = self.part(slot, owner, first, last)
        here = self.part(slot, owner, first, last, self.own) if mine else there
        group = self.line if mine and slot == self.pair else zs
        return pltpu.make_async_remote_copy(
            src_ref=here,
            dst_ref=there,
            send_sem=self.side_send.at[group],
            recv_sem=self.side_recv.at[group],
            device_id={"rows": self.z * SIDE + 1 - self.y},
            device_id_type=MESH,
        )

    def both_ways(self, c):
        z = self.z

        @pl.when(z > 0)
        def _():
            self.to_line(z, c, False, z - 1, True, True).start()

        @pl.when(z < self.line - 1)
        def _():
            self.to_line(z, c, True, z + 1, True, True).start()

    def send_own(self, slot):
        for c, chunk in enumerate(self.chunks):
            if chunk[0] == slot and not chunk[3]:
                self.both_ways(c)
        self.to_side(self.z, slot, self.skip if slot == 0 else 0, mine=True).start()

    def pass_on(self, d, c):
        z, line = self.z, self.line
        slot, first, last, _ = self.chunks[c]

        @pl.when(z - d >= 0)
        def _():
            self.to_line(z - d, c, True, z, d == 1).wait_recv()

            @pl.when(z < line - 1)
            def _():
                self.to_line(z - d, c, True, z + 1).start()

            if c < self.spread:
                self.to_side(z - d, slot, first, last=last).start()

        @pl.when(z + d < line)
        def _():
            self.to_line(z + d, c, False, z, d == 1).wait_recv()

            @pl.when(z > 0)
            def _():
                self.to_line(z + d, c, False, z - 1).start()

            if c < self.spread:
                self.to_side(z + d, slot, first, last=last).start()

    def relay(self):
        crossed = len(self.chunks) - 1
        for d in range(1, self.line):
            for c in range(crossed):
                self.pass_on(d, c)
            if d == 1:
                self.to_side(self.z, self.pair, 0, False, True).wait_recv()
                self.both_ways(crossed)
        for d in range(1, self.line):
            self.pass_on(d, crossed)

    def finish(self):
        z, line, share, count, cut = self.z, self.line, self.share, self.count, self.cut
        full = count * share + cut

        @pl.when(z > 0)
        def _():
            wait_bytes(self.some(full - self.skip), self.own_send.at[0])

        @pl.when(z < line - 1)
        def _():
            wait_bytes(self.some(full - self.skip), self.own_send.at[1])

        self.to_side(z, self.pair, 0, mine=True).wait_send()
        for zs in range(line):

            @pl.when((z > 0) & (z < zs))
            def _():
                wait_bytes(self.some(full), self.down_send.at[zs])

            @pl.when((z < line - 1) & (z > zs))
            def _():
                wait_bytes(self.some(full), self.up_send.at[zs])

            for sem in (self.side_recv, self.side_send):

                if count > 1:

                    @pl.when(z == zs)
                    def _():
                        wait_bytes(self.some((count - 1) * share - self.skip), sem.at[zs])

                @pl.when(z != zs)
                def _():
                    wait_bytes(self.some(count * share - cut), sem.at[zs])


def cut_of(line, share, count):
    return max(32, round(count * share / (2 * (line - 1)) / 32) * 32)


def gather_sems(line, most):
    dma = pltpu.SemaphoreType.DMA
    return [dma((2,)), dma((line,)), dma((line,)), dma((line + 1,)),
            dma((line - 1, most + 3)), dma((line + 1,))]


def opening(n_rows, n_model, blocks, orders, d_model, *refs):
    ins, refs = refs[:9], refs[9:]
    nt_ref, ns_ref = refs[:2]
    whole, later, cols, norm_out, results = refs[2], refs[3], refs[4:7], refs[7], refs[8:11]
    bufs = refs[11:14]
    (norms, lines, sums, gains, in_sem, norm_sem, sum_send, sum_recv, gain_send, gain_recv,
     early, early_send, early_recv) = refs[14:27]
    sems = refs[27:]

    line = n_rows // SIDE
    me = lax.axis_index("rows")
    col = lax.axis_index("model")
    z, y = me // SIDE, me % SIDE
    other = 1 - y
    share = bufs[0].shape[1]
    width = blocks[0][2]

    half = share // 2

    def load(b, rows=pl.ds(0, share), sem=None):
        a, start, _ = blocks[b]
        where = (rows, pl.ds(start, width))
        for k in range(3):
            pltpu.make_async_copy(
                ins[3 * a + k].at[where],
                bufs[a].at[(k, *where)],
                in_sem.at[b if sem is None else sem],
            ).start()

    def load_first(core):
        b = orders[core][0][0]
        load(b, pl.ds(0, half), len(blocks))
        load(b, pl.ds(half, half))

    on_core(load_first)
    barrier = pltpu.get_barrier_semaphore()
    for k in range(1, n_rows):
        pl.semaphore_signal(
            barrier, inc=1, device_id={"rows": lax.rem(me + k, n_rows)}, device_id_type=MESH
        )
    for k in range(1, n_model):
        pl.semaphore_signal(
            barrier, inc=1, device_id={"model": lax.rem(col + k, n_model)}, device_id_type=MESH
        )

    def step(b, rest=()):
        a, start, _ = blocks[b]
        def one(i, acc):
            rows = pl.ds(pl.multiple_of(i * TILE, TILE), TILE)
            where = (rows, pl.ds(start, width))
            r = adam(*(bufs[a][(k, *where)] for k in range(3)))
            results[a][where] = r
            m = jnp.abs(r).reshape(TILE // 8, 8, width)
            return acc + jnp.sum(m, axis=0)

        acc, done = jnp.zeros((8, width), jnp.float32), 0
        if rest:
            wait_bytes(bufs[a].at[:, pl.ds(0, half), pl.ds(start, width)], in_sem.at[len(blocks)])
            done = half
            acc = lax.fori_loop(0, done // TILE, one, acc)
        wait_bytes(
            bufs[a].at[:, pl.ds(done, share - done), pl.ds(start, width)], in_sem.at[b]
        )
        if rest:
            for r in rest:
                load(r)
            for n, ref in enumerate((nt_ref, ns_ref)):
                pltpu.make_async_copy(ref, norms.at[n], norm_sem.at[0]).start()

        acc = lax.fori_loop(done // TILE, share // TILE, one, acc)
        sums[b, me] = jnp.sum(acc, axis=0, keepdims=True)

    def sum_copy(b, k):
        return pltpu.make_async_remote_copy(
            src_ref=sums.at[b, me],
            dst_ref=sums.at[b, me],
            send_sem=sum_send.at[0],
            recv_sem=sum_recv.at[b],
            device_id={"rows": lax.rem(me + k, n_rows)},
            device_id_type=MESH,
        )

    def early_copy(b, n, to, rows):
        a, start, _ = blocks[b]
        return pltpu.make_async_remote_copy(
            src_ref=results[a].at[pl.ds(0, rows), pl.ds(start, width)],
            dst_ref=early.at[n, pl.ds(0, rows)],
            send_sem=early_send.at[n],
            recv_sem=early_recv.at[n],
            device_id={"rows": to},
            device_id_type=MESH,
        )

    def gain_model(k):
        return pltpu.make_async_remote_copy(
            src_ref=gains.at[me, col],
            dst_ref=gains.at[me, col],
            send_sem=gain_send.at[0],
            recv_sem=gain_recv.at[0],
            device_id={"model": lax.rem(col + k, n_model)},
            device_id_type=MESH,
        )

    def gain_rows(k):
        return pltpu.make_async_remote_copy(
            src_ref=gains.at[me],
            dst_ref=gains.at[me],
            send_sem=gain_send.at[1],
            recv_sem=gain_recv.at[1],
            device_id={"rows": lax.rem(me + k, n_rows)},
            device_id_type=MESH,
        )

    def work(core):
        now, then = orders[core]
        order = now + then
        ahead = EARLY[core]
        gather = Gather(n_rows, share, width, len(now), ahead, whole, None, sems)
        for i, b in enumerate(order):
            step(b, order[1:] if i == 0 else ())
            if i == 0:
                pl.semaphore_wait(barrier, n_rows + n_model - 2)
            for k in range(1, n_rows):
                sum_copy(b, k).start()
            if i == 0 and ahead:
                early_copy(b, 0, z * SIDE + other, ahead).start()

                @pl.when(z < line - 1)
                def _():
                    early_copy(b, 1, me + SIDE, ahead).start()

                @pl.when(z > 0)
                def _():
                    early_copy(b, 2, me - SIDE, ahead).start()

        wait_bytes(norms, norm_sem.at[0])
        gains[me, col] = norms[0] + norms[1]
        for k in range(1, n_model):
            gain_model(k).start()

        for i, b in enumerate(order):
            a, start, _ = blocks[b]
            wait_bytes(sums.at[b, pl.ds(0, n_rows - 1)], sum_recv.at[b])
            total = sums[b, 0]
            for k in range(1, n_rows):
                total = total + sums[b, k]
            column = total / d_model
            cols[a][:, pl.ds(start, width)] = column
            scale = jnp.broadcast_to(1.0 / column, (TILE, width))
            mine = i < len(now)
            slot = i if mine else i - len(now)

            def one(t, carry):
                rows = pl.ds(pl.multiple_of(t * TILE, TILE), TILE)
                value = (results[a][rows, pl.ds(start, width)] * scale).astype(jnp.bfloat16)
                where = pl.ds(slot * width, width)
                if mine:
                    whole[pl.ds(pl.multiple_of(me * share + t * TILE, TILE), TILE), where] = value
                else:
                    later[rows, where] = value
                return carry

            lax.fori_loop(0, share // TILE, one, 0)
            if mine:
                gather.send_own(slot)

        if ahead:
            a, start, _ = blocks[order[0]]
            scale = jnp.broadcast_to(1.0 / cols[a][:, pl.ds(start, width)], (TILE, width))

            def scaled(n, owner):
                early_copy(order[0], n, owner, ahead).wait_recv()

                def one(t, carry):
                    rows = pl.ds(pl.multiple_of(t * TILE, TILE), TILE)
                    there = pl.ds(pl.multiple_of(owner * share + t * TILE, TILE), TILE)
                    whole[there, pl.ds(0, width)] = (early[n, rows] * scale).astype(jnp.bfloat16)
                    return carry

                lax.fori_loop(0, ahead // TILE, one, 0)

            @pl.when(z > 0)
            def _():
                scaled(1, me - SIDE)

            @pl.when(z < line - 1)
            def _():
                scaled(2, me + SIDE)

            scaled(0, z * SIDE + other)

        wait_bytes(gains.at[0, pl.ds(0, n_model - 1)], gain_recv.at[0])
        for k in range(1, n_rows):
            gain_rows(k).start()
        gather.relay()
        if ahead:
            early_copy(order[0], 0, me, ahead).wait_send()

            @pl.when(z < line - 1)
            def _():
                early_copy(order[0], 1, me, ahead).wait_send()

            @pl.when(z > 0)
            def _():
                early_copy(order[0], 2, me, ahead).wait_send()

        gather.finish()

    on_core(work)
    wait_bytes(gains.at[pl.ds(0, n_rows - 1)], gain_recv.at[1])
    for r in range(n_rows):
        for m in range(n_model):
            lines[pl.ds(r * n_model + m, 1), :] = gains[r, m]
    norm_out[...] = lines[...].astype(jnp.bfloat16)
    wait_bytes(gains.at[0, pl.ds(0, n_model - 1)], gain_send.at[0])
    wait_bytes(gains.at[pl.ds(0, n_rows - 1)], gain_send.at[1])
    wait_bytes(sums.at[:, pl.ds(0, n_rows - 1)], sum_send.at[0])


def closing(n_rows, blocks, orders, own, token, whole, *sems):
    line = n_rows // SIDE
    me = lax.axis_index("rows")
    z, y = me // SIDE, me % SIDE
    share, width = own.shape[0], blocks[0][2]
    barrier = pltpu.get_barrier_semaphore()

    def signal(who):
        pl.semaphore_signal(barrier, inc=1, device_id={"rows": who}, device_id_type=MESH)

    signal(z * SIDE + 1 - y)

    @pl.when(z > 0)
    def _():
        signal(me - SIDE)

    @pl.when(z < line - 1)
    def _():
        signal(me + SIDE)

    pl.semaphore_wait(barrier, 1 + jnp.where(z > 0, 1, 0) + jnp.where(z < line - 1, 1, 0))

    def work(core):
        count = len(orders[core][1])
        gather = Gather(n_rows, share, width, count, 0, whole, own, sems)
        for slot in range(count):
            gather.send_own(slot)

        def one(t, carry):
            rows = pl.ds(pl.multiple_of(t * TILE, TILE), TILE)
            there = pl.ds(pl.multiple_of(me * share + t * TILE, TILE), TILE)
            whole[there, pl.ds(0, count * width)] = own[rows, pl.ds(0, count * width)]
            return carry

        lax.fori_loop(0, share // TILE, one, 0)
        gather.relay()
        gather.finish()

    on_core(work)


def put(blocks, orders, phase, whole, finals, sem):
    def work(core):
        copies = []
        for slot, b in enumerate(orders[core][phase]):
            a, start, width = blocks[b]
            c = pltpu.make_async_copy(
                whole.at[:, pl.ds(slot * width, width)],
                finals[a].at[:, pl.ds(start, width)],
                sem.at[slot],
            )
            c.start()
            copies.append(c)
        for c in copies:
            c.wait()

    on_core(work)


def write(blocks, orders, *refs):
    whole, small, finals, outs, token, sem = refs[0], refs[1:8], refs[8:11], refs[11:18], refs[18], refs[19]
    most = max(len(o) for c in orders for o in c)
    copies = []
    for n, (src, dst) in enumerate(zip(small, outs)):
        c = pltpu.make_async_copy(src, dst, sem.at[most + n])
        c.start()
        copies.append(c)
    token[...] = jnp.zeros_like(token)
    put(blocks, orders, 0, whole, finals, sem)
    for c in copies:
        c.wait()


def rest(blocks, orders, whole, *refs):
    put(blocks, orders, 1, whole, refs[3:6], refs[6])


def fused(n_rows, n_model, d_model, blocks, arrays):
    *weights, norm_train, norm_step = arrays
    share = weights[0].shape[0]
    widths = [weights[3 * a].shape[1] for a in range(3)]
    line, nb, width = n_rows // SIDE, len(blocks), blocks[0][2]
    unit = norm_train.shape[0]
    big = [b for b in range(nb) if blocks[b][0] == 0]
    few = [b for b in range(nb) if blocks[b][0] != 0]
    orders = ((big, few), (few, big))
    most = [max(len(orders[c][p]) for c in range(2)) for p in range(2)]
    anywhere = pl.BlockSpec(memory_space=pl.ANY)
    vmem = pl.BlockSpec(memory_space=pltpu.VMEM)
    f32, b16, dma = jnp.float32, jnp.bfloat16, pltpu.SemaphoreType.DMA
    whole, own, *small = pl.pallas_call(
        functools.partial(opening, n_rows, n_model, blocks, orders, d_model),
        out_shape=[
            pltpu.VMEM((d_model, most[0] * width), b16),
            pltpu.VMEM((share, most[1] * width), b16),
            *(pltpu.VMEM((1, w), f32) for w in widths),
            pltpu.VMEM((n_rows * n_model, unit), b16),
            *(pltpu.VMEM((share, w), f32) for w in widths),
        ],
        in_specs=[anywhere] * 11,
        out_specs=[vmem] * 9,
        scratch_shapes=[
            *(pltpu.VMEM((3, share, w), f32) for w in widths),
            pltpu.VMEM((2, 1, unit), f32),
            pltpu.VMEM((n_rows * n_model, unit), f32),
            pltpu.VMEM((nb, n_rows, 1, width), f32),
            pltpu.VMEM((n_rows, n_model, 1, unit), f32),
            dma((nb + 1,)),
            dma((1,)),
            dma((1,)),
            dma((nb,)),
            dma((2,)),
            dma((2,)),
            pltpu.VMEM((3, max(EARLY), width), f32),
            dma((3,)),
            dma((3,)),
            *gather_sems(line, most[0]),
        ],
        compiler_params=pltpu.CompilerParams(
            collective_id=0, has_side_effects=True, vmem_limit_bytes=49 * 2**20
        ),
    )(*weights, norm_train.reshape(1, -1), norm_step.reshape(1, -1))
    *finals, c0, c1, c2, serve, r0, r1, r2, token = pl.pallas_call(
        functools.partial(write, blocks, orders),
        out_shape=[
            *(jax.ShapeDtypeStruct((d_model, w), b16) for w in widths),
            *(jax.ShapeDtypeStruct(o.shape, o.dtype) for o in small),
            pltpu.VMEM((8, 128), f32),
        ],
        in_specs=[anywhere] * 8,
        out_specs=[anywhere] * 10 + [vmem],
        scratch_shapes=[dma((max(most) + 7,))],
        compiler_params=pltpu.CompilerParams(vmem_limit_bytes=2**20),
    )(whole, *small)
    whole = pl.pallas_call(
        functools.partial(closing, n_rows, blocks, orders),
        out_shape=pltpu.VMEM((d_model, most[1] * width), b16),
        in_specs=[vmem, anywhere],
        out_specs=vmem,
        scratch_shapes=gather_sems(line, most[1]),
        compiler_params=pltpu.CompilerParams(
            collective_id=1, has_side_effects=True, vmem_limit_bytes=40 * 2**20
        ),
    )(own, token)
    finals = pl.pallas_call(
        functools.partial(rest, blocks, orders),
        out_shape=[jax.ShapeDtypeStruct((d_model, w), b16) for w in widths],
        in_specs=[anywhere] * 4,
        out_specs=[anywhere] * 3,
        scratch_shapes=[dma((most[1],))],
        input_output_aliases={1: 0, 2: 1, 3: 2},
        compiler_params=pltpu.CompilerParams(vmem_limit_bytes=2**20),
    )(whole, *finals)
    return (*finals, *(d.reshape(-1) for d in (c0, c1, c2, serve)), r0, r1, r2)


def solution(mesh):
    n_rows, n_model = mesh.shape["rows"], mesh.shape["model"]

    def body(*arrays):
        share = arrays[0].shape[0]
        widths = [arrays[3 * a].shape[1] for a in range(3)]
        width = min(widths)
        d_model = share * n_rows
        line = n_rows // SIDE
        counts = (1, widths[0] // width, (widths[0] + widths[1] + widths[2]) // width - 1)
        fits = (
            n_rows % SIDE == 0
            and n_model % 2 == 0
            and 2 <= line <= 4
            and share % (2 * TILE) == 0
            and share > max(EARLY)
            and width % 128 == 0
            and all(w % width == 0 for w in widths)
            and counts[1] > 1
            and all(cut_of(line, share, c) <= share - 64 for c in counts)
        )
        if not fits:
            return plain(d_model, arrays)
        blocks = tuple(
            (a, s, width) for a, w in enumerate(widths) for s in range(0, w, width)
        )
        return fused(n_rows, n_model, d_model, blocks, arrays)

    return jax.shard_map(
        body,
        mesh=mesh,
        in_specs=(P("rows", "model"),) * 9 + (P(("rows", "model")),) * 2,
        out_specs=(
            *(P(None, "model"),) * 3,
            *(P("model"),) * 3,
            P(),
            *(P("rows", "model"),) * 3,
        ),
        check_vma=False,
    )
```
